16 devices in a mesh: dp: 2 (over y, z), ep: 8 (over x, core).
Axes of the slice: x: 4, y: 2, z: 1, core: 2. Of those that a mesh axis runs over, the one named last changes fastest.
The devices are a block of a 4x4x8 slice.
Arguments:
- hidden_in: bfloat16 [768, 1536], P(('dp', 'ep')), parts along dimension 0
- norm_gain: float32 [1536], replicated
- router_w: float32 [64, 1536], replicated
- w_gate: bfloat16 [64, 1536, 512], P('ep')
- w_up: bfloat16 [64, 1536, 512], P('ep')
- w_down: bfloat16 [64, 512, 1536], P('ep')
- ws_gate: bfloat16 [1536, 1024], replicated
- ws_up: bfloat16 [1536, 1024], replicated
- ws_down: bfloat16 [1024, 1536], replicated
- expert_ids: int32 [768, 6], P(('dp', 'ep')), parts along dimension 0
Outputs:
- output: bfloat16 [768, 1536], P(('dp', 'ep')), parts along dimension 0
There are 2 independent parts. The reference program is written for one: setup_inputs(seed, part) draws one part's arguments, and reference() takes and returns one part's arrays. A program takes and returns all parts, laid end to end along the dimension named above; an argument that names none is the same for every part.
All inputs are finite; a program needn't handle non-finite values.
Results may differ from the reference program's by a relative error of at most 0.00425754.
Values are sent between devices in bfloat16 or wider.
A program may use at most 768 MiB of HBM per device.

```python
import jax
import jax.numpy as jnp
from jax import lax

TOKENS = 384
D = 1536
EXPERTS = 64
INTER = 512
SHARED_INTER = 1024
TOP = 6
GROUPS = 8
GROUP_LIMIT = 4

NORM_EPS = 1e-6
ROUTE_SCALE = 2.5
GROUP_WIDTH = EXPERTS // GROUPS
SLOT_PAIRS = (TOP + GROUP_LIMIT - 1) // GROUP_LIMIT
EXP_CAP = GROUPS * SLOT_PAIRS * TOKENS // EXPERTS


def draw_routes(route_key):
    key_hot, key_other, key_shift, key_cols = jax.random.split(route_key, 4)
    slot_sizes = [TOP // GROUP_LIMIT + int(slot_num < TOP % GROUP_LIMIT) for slot_num in range(GROUP_LIMIT)]
    slot_of_pair = jnp.array([slot_num for slot_num in range(GROUP_LIMIT) for step_num in range(slot_sizes[slot_num])], jnp.int32)
    step_of_pair = jnp.array([step_num for slot_num in range(GROUP_LIMIT) for step_num in range(slot_sizes[slot_num])], jnp.int32)
    hot_group = jax.random.randint(key_hot, (), 0, GROUPS).astype(jnp.int32)
    other_scores = jax.random.randint(key_other, (TOKENS, GROUPS - 1), 0, 1 << 20).astype(jnp.int32) * (GROUPS - 1) + jnp.arange(GROUPS - 1, dtype=jnp.int32)
    other_offsets = jnp.argsort(other_scores, axis=1)[:, : GROUP_LIMIT - 1].astype(jnp.int32)
    token_groups = jnp.concatenate([jnp.zeros((TOKENS, 1), jnp.int32) + hot_group, (hot_group + 1 + other_offsets) % GROUPS], axis=1)
    pair_groups = token_groups[:, slot_of_pair]
    group_shift = jax.random.randint(key_shift, (GROUPS,), 0, GROUP_WIDTH).astype(jnp.int32)
    token_pos = jnp.arange(TOKENS, dtype=jnp.int32)[:, None]
    within = (token_pos + step_of_pair[None, :] + group_shift[pair_groups]) % GROUP_WIDTH
    routes = pair_groups * GROUP_WIDTH + within
    col_scores = jax.random.randint(key_cols, (TOKENS, TOP), 0, 1 << 20).astype(jnp.int32) * TOP + jnp.arange(TOP, dtype=jnp.int32)
    col_order = jnp.argsort(col_scores, axis=1)
    return jnp.take_along_axis(routes, col_order, axis=1).astype(jnp.int32)


def setup_inputs(seed: int = 0, part: int = 0) -> dict:
    base_key = jax.random.key(seed)
    weight_keys = jax.random.split(base_key, 9)
    part_keys = jax.random.split(jax.random.fold_in(base_key, part), 2)
    hidden_in = jax.random.normal(part_keys[0], (TOKENS, D), jnp.float32).astype(jnp.bfloat16)
    expert_ids = draw_routes(part_keys[1])
    norm_gain = jax.random.uniform(weight_keys[0], (D,), jnp.float32, 0.5, 1.5)
    router_w = jax.random.normal(weight_keys[1], (EXPERTS, D), jnp.float32) * D ** -0.5
    w_gate = (jax.random.normal(weight_keys[2], (EXPERTS, D, INTER), jnp.float32) * D ** -0.5).astype(jnp.bfloat16)
    w_up = (jax.random.normal(weight_keys[3], (EXPERTS, D, INTER), jnp.float32) * D ** -0.5).astype(jnp.bfloat16)
    out_scale = jax.random.uniform(weight_keys[4], (EXPERTS, 1, 1), jnp.float32, 1.0, 3.0)
    w_down = (jax.random.normal(weight_keys[5], (EXPERTS, INTER, D), jnp.float32) * INTER ** -0.5 * out_scale).astype(jnp.bfloat16)
    ws_gate = (jax.random.normal(weight_keys[6], (D, SHARED_INTER), jnp.float32) * D ** -0.5).astype(jnp.bfloat16)
    ws_up = (jax.random.normal(weight_keys[7], (D, SHARED_INTER), jnp.float32) * D ** -0.5).astype(jnp.bfloat16)
    ws_down = (jax.random.normal(weight_keys[8], (SHARED_INTER, D), jnp.float32) * SHARED_INTER ** -0.5).astype(jnp.bfloat16)
    return {"hidden_in": hidden_in, "norm_gain": norm_gain, "router_w": router_w, "w_gate": w_gate, "w_up": w_up, "w_down": w_down, "ws_gate": ws_gate, "ws_up": ws_up, "ws_down": ws_down, "expert_ids": expert_ids}


def swiglu(tok_rows, gate_mat, up_mat, down_mat):
    h_gate = jnp.dot(tok_rows, gate_mat, preferred_element_type=jnp.float32)
    h_up = jnp.dot(tok_rows, up_mat, preferred_element_type=jnp.float32)
    hidden = (jax.nn.silu(h_gate) * h_up).astype(jnp.bfloat16)
    return jnp.dot(hidden, down_mat, preferred_element_type=jnp.float32).astype(jnp.bfloat16)


def reference(hidden_in, norm_gain, router_w, w_gate, w_up, w_down, ws_gate, ws_up, ws_down, expert_ids):
    x_f32 = hidden_in.astype(jnp.float32)
    inv_rms = lax.rsqrt(jnp.mean(x_f32 * x_f32, axis=1, keepdims=True) + NORM_EPS)
    x_norm = (x_f32 * inv_rms * norm_gain).astype(jnp.bfloat16)
    scores = jax.nn.sigmoid(jnp.dot(x_norm.astype(jnp.float32), router_w.T))
    picked = jnp.take_along_axis(scores, expert_ids, axis=1)
    gate_vals = ROUTE_SCALE * picked / jnp.sum(picked, axis=1, keepdims=True)
    flat_ids = expert_ids.reshape(-1)
    pair_tok = jnp.arange(TOKENS * TOP, dtype=jnp.int32) // TOP
    sort_order = jnp.argsort(flat_ids)
    counts = jnp.bincount(flat_ids, length=EXPERTS).astype(jnp.int32)
    starts = jnp.cumsum(counts) - counts
    sorted_tok = jnp.concatenate([pair_tok[sort_order], jnp.full((EXP_CAP,), TOKENS, jnp.int32)])
    norm_pad = jnp.concatenate([x_norm, jnp.zeros((1, D), x_norm.dtype)], axis=0)

    def one_expert(expert_xs):
        gate_mat, up_mat, down_mat, row_start, row_count = expert_xs
        row_tok = lax.dynamic_slice(sorted_tok, (row_start,), (EXP_CAP,))
        row_tok = jnp.where(jnp.arange(EXP_CAP, dtype=jnp.int32) < row_count, row_tok, TOKENS)
        return swiglu(norm_pad[row_tok], gate_mat, up_mat, down_mat)

    expert_out = lax.map(one_expert, (w_gate, w_up, w_down, starts, counts))
    sorted_rank = (jnp.arange(TOKENS * TOP, dtype=jnp.int32) - starts[flat_ids[sort_order]]).astype(jnp.int32)
    pair_rank = jnp.zeros((TOKENS * TOP,), jnp.int32).at[sort_order].set(sorted_rank)
    pair_out = expert_out[flat_ids, pair_rank].reshape(TOKENS, TOP, D)
    routed = jnp.sum(gate_vals[:, :, None] * pair_out.astype(jnp.float32), axis=1)
    shared_out = swiglu(x_norm, ws_gate, ws_up, ws_down)
    return (x_f32 + shared_out.astype(jnp.float32) + routed).astype(jnp.bfloat16)
```

```python
import functools

import jax
import jax.numpy as jnp
from jax import lax
from jax.experimental import pallas as pl
from jax.experimental.pallas import tpu as pltpu
from jax.sharding import PartitionSpec as P

NORM_EPS = 1e-6
ROUTE_SCALE = 2.5
GROUPS = 8
GROUP_LIMIT = 4
CORES = 2
COLS = 256
MESH = pl.DeviceIdType.MESH
F32 = jnp.float32
BF16 = jnp.bfloat16


def dot(a, b):
    return jnp.dot(a, b, preferred_element_type=F32)


def dot_t(a, b):
    return lax.dot_general(a, b, (((1,), (1,)), ((), ())), preferred_element_type=F32)


def split3(v):
    hi = v.astype(BF16)
    rest = v - hi.astype(F32)
    mid = rest.astype(BF16)
    low = (rest - mid.astype(F32)).astype(BF16)
    return hi, mid, low


def moe_kernel(ep_size, cap, hid_h, gain_h, rw_h, wg_h, wu_h, wd_h, sg_h, su_h, sd_h, ids_h, out_ref,
               hid, gain, rw, ids, wg, wu, wd, sg, su, sd, x_all, gt_send, gt_all, p_all, ga, a_hi, a_mid, a_low,
               xg, hbuf, ybuf, sbuf, d2d, tbuf, hopa, hopb, rela, relb, froml, fromr, hsh, shared,
               in_sem, w_sem, send_sem, recv_sem):
    chips = ep_size // CORES
    tok, dim = hid.shape
    n_exp, _, inter = wg.shape
    top_k = ids.shape[0]
    half = dim // 2
    rows = ep_size * tok
    n_blk = dim // COLS
    hc = COLS // 2

    me = lax.axis_index("ep")
    chip, core = me // CORES, me % CORES
    other = 1 - core
    right, left, opp = (chip + 1) % chips, (chip + chips - 1) % chips, (chip + 2) % chips

    def slot(a_chip, a_core):
        return a_core * chips + a_chip

    def dev(a_chip, a_core):
        return {"ep": a_chip * CORES + a_core}

    used = [0]

    def remote(src, dst, to):
        i = used[0]
        used[0] += 1
        copy = pltpu.make_async_remote_copy(src, dst, send_sem.at[i], recv_sem.at[i], device_id=to, device_id_type=MESH)
        copy.start()
        sent.append(copy)
        return copy

    sent = []

    ins = [pltpu.make_async_copy(s, d, in_sem.at[i]) for i, (s, d) in enumerate(((hid_h, hid), (gain_h, gain), (rw_h, rw), (ids_h, ids)))]
    for copy in ins:
        copy.start()
    wcopies = {}

    def fetch(key, s, d):
        copy = pltpu.make_async_copy(s, d, w_sem.at[len(wcopies)])
        copy.start(priority=1)
        wcopies[key] = copy

    for e in range(n_exp):
        fetch(("g", e), wg_h.at[e], wg.at[e])
        fetch(("u", e), wu_h.at[e], wu.at[e])
    for e in range(n_exp):
        fetch(("d", e), wd_h.at[e], wd.at[e])
    fetch("sg", sg_h, sg)
    fetch("su", su_h, su)
    fetch("sd", sd_h, sd)

    barrier = pltpu.get_barrier_semaphore()
    for k in range(1, ep_size):
        pl.semaphore_signal(barrier, inc=1, device_id={"ep": (me + k) % ep_size}, device_id_type=MESH)

    mine = slot(chip, core)
    ins[0].wait()
    ins[1].wait()
    x_f32 = hid[...].astype(F32)
    inv_rms = lax.rsqrt(jnp.mean(x_f32 * x_f32, axis=-1, keepdims=True) + NORM_EPS)
    x_norm = (x_f32 * inv_rms * gain[...]).astype(BF16)
    x_all[mine] = x_norm

    pl.semaphore_wait(barrier, ep_size - 1)

    part_a, part_b = slice(0, half), slice(half, dim)

    def spread(a_slot, cols, to):
        ref = x_all.at[a_slot, :, cols]
        return remote(ref, ref, to)

    ra = spread(mine, part_a, dev(right, core))
    lb = spread(mine, part_b, dev(left, core))
    rb = spread(mine, part_b, dev(right, core))
    la = spread(mine, part_a, dev(left, core))
    cross = [spread(mine, slice(0, dim), dev(chip, other))]

    ins[2].wait()
    ins[3].wait()
    r_hi, r_mid, r_low = split3(rw[...])
    logits = (dot_t(r_low, x_norm) + dot_t(r_mid, x_norm)) + dot_t(r_hi, x_norm)
    scores = 1.0 / (1.0 + jnp.exp(-logits))
    exp_no = lax.broadcasted_iota(jnp.int32, logits.shape, 0)
    chosen = exp_no == ids[0:1, :]
    for k in range(1, top_k):
        chosen = jnp.logical_or(chosen, exp_no == ids[k : k + 1, :])
    total = jnp.sum(jnp.where(chosen, scores, 0.0), axis=0, keepdims=True)
    gates = jnp.where(chosen, ROUTE_SCALE * scores / total, -1.0)
    gt_send[...] = jnp.full(gt_send.shape, -1.0, F32)
    for d in range(ep_size):
        gt_send[d, :, 0:tok] = gates[d * n_exp : (d + 1) * n_exp, :]
    gt_all[mine] = gt_send[me]
    tiles = []
    for k in range(1, ep_size):
        to = (me + k) % ep_size
        tiles.append(remote(gt_send.at[to], gt_all.at[mine], {"ep": to}))

    ra.wait_recv()
    fa = spread(slot(left, core), part_a, dev(right, core))
    cross.append(spread(slot(left, core), part_a, dev(chip, other)))
    lb.wait_recv()
    fb = spread(slot(right, core), part_b, dev(left, core))
    cross.append(spread(slot(right, core), part_b, dev(chip, other)))
    rb.wait_recv()
    cross.append(spread(slot(left, core), part_b, dev(chip, other)))
    la.wait_recv()
    cross.append(spread(slot(right, core), part_a, dev(chip, other)))

    for copy in tiles:
        copy.wait_recv()
    lane_src = lax.broadcasted_iota(jnp.int32, (n_exp, rows), 1) // tok
    gmat = jnp.full((n_exp, rows), -1.0, F32)
    for s in range(ep_size):
        wide = jnp.concatenate([gt_all[s], jnp.full((n_exp, rows - gt_all.shape[2]), -1.0, F32)], axis=1)
        if s:
            wide = pltpu.roll(wide, s * tok, 1)
        gmat = jnp.where(lane_src == s, wide, gmat)
    picked = jnp.logical_not(gmat < 0.0)
    upper = lax.broadcasted_iota(jnp.int32, (rows, rows), 0) < lax.broadcasted_iota(jnp.int32, (rows, rows), 1)
    rank = dot(jnp.where(picked, 1.0, 0.0).astype(BF16), jnp.where(upper, 1.0, 0.0).astype(BF16))
    place = jnp.where(picked, rank, -1.0)
    row_no = lax.broadcasted_iota(jnp.int32, (cap, rows), 0).astype(F32)
    for e in range(n_exp):
        hit = row_no == place[e : e + 1, :]
        p_all[e * cap : (e + 1) * cap, :] = jnp.where(hit, 1.0, 0.0).astype(BF16)
        ga[e * cap : (e + 1) * cap, :] = jnp.where(hit, gmat[e : e + 1, :], 0.0)
    for i in range(n_exp * cap // 128):
        lanes = slice(i * 128, (i + 1) * 128)
        hi, mid, low = split3(ga[lanes, :].T)
        a_hi[:, lanes] = hi
        a_mid[:, lanes] = mid
        a_low[:, lanes] = low

    fa.wait_recv()
    cross.append(spread(slot(opp, core), part_a, dev(chip, other)))
    fb.wait_recv()
    cross.append(spread(slot(opp, core), part_b, dev(chip, other)))
    for copy in cross:
        copy.wait_recv()

    x_rows = x_all[...].reshape(rows, dim)
    for e in range(0, n_exp, 2):
        two = slice(e * cap, (e + 2) * cap)
        xg[two, :] = dot(p_all[two, :], x_rows).astype(BF16)
    for e in range(n_exp):
        own = slice(e * cap, (e + 1) * cap)
        wcopies[("g", e)].wait()
        wcopies[("u", e)].wait()
        h_gate = dot(xg[own, :], wg[e])
        h_up = dot(xg[own, :], wu[e])
        hbuf[own, :] = (jax.nn.silu(h_gate) * h_up).astype(BF16)
    for e in range(n_exp):
        wcopies[("d", e)].wait()

    part = []

    def compute(j):
        cols = slice(j * COLS, (j + 1) * COLS)
        for e in range(n_exp):
            own = slice(e * cap, (e + 1) * cap)
            ybuf[own, :] = dot(hbuf[own, :], wd[e, :, cols]).astype(BF16)
        y = ybuf[...]
        s = (dot(a_low[...], y) + dot(a_mid[...], y)) + dot(a_hi[...], y)
        sbuf[j] = s.reshape(CORES, chips * tok, COLS)
        part.append({"d2d": remote(sbuf.at[j, other], d2d.at[j], dev(chip, other))})

    lo, up = slice(0, hc), slice(hc, COLS)

    def send(j):
        part[j]["d2d"].wait_recv()
        tbuf[j] = (sbuf[j, core] + d2d[j]).reshape(chips, tok, COLS)
        part[j]["ha"] = remote(tbuf.at[j, opp, :, lo], hopa.at[j], dev(right, core))
        part[j]["hb"] = remote(tbuf.at[j, opp, :, up], hopb.at[j], dev(left, core))
        part[j]["db"] = remote(tbuf.at[j, right, :, up], froml.at[j, :, up], dev(right, core))
        part[j]["da"] = remote(tbuf.at[j, left, :, lo], fromr.at[j, :, lo], dev(left, core))

    def relay(j):
        part[j]["ha"].wait_recv()
        rela[j] = hopa[j] + tbuf[j, right, :, lo]
        part[j]["ra"] = remote(rela.at[j], froml.at[j, :, lo], dev(right, core))
        part[j]["hb"].wait_recv()
        relb[j] = hopb[j] + tbuf[j, left, :, up]
        part[j]["rb"] = remote(relb.at[j], fromr.at[j, :, up], dev(left, core))

    def finish(j):
        for key in ("db", "da", "ra", "rb"):
            part[j][key].wait_recv()
        cols = slice(j * COLS, (j + 1) * COLS)
        routed = (tbuf[j, chip] + froml[j]) + fromr[j]
        out_ref[:, cols] = ((hid[:, cols].astype(F32) + shared[:, cols].astype(F32)) + routed).astype(BF16)

    for j in range(n_blk):
        compute(j)
        if j >= 1:
            send(j - 1)
        if j >= 3:
            relay(j - 3)
    send(n_blk - 1)
    relay(n_blk - 3)

    wcopies["sg"].wait()
    wcopies["su"].wait()
    wcopies["sd"].wait()
    xs = x_all[mine]
    mid_cols = hsh.shape[1] // 2
    for k in range(2):
        cols = slice(k * mid_cols, (k + 1) * mid_cols)
        hsh[:, cols] = (jax.nn.silu(dot(xs, sg[:, cols])) * dot(xs, su[:, cols])).astype(BF16)
        relay(n_blk - 2 + k)
    shared[...] = dot(hsh[...], sd[...]).astype(BF16)
    for j in range(n_blk):
        finish(j)
    for copy in sent:
        copy.wait_send()


def solution(mesh):
    ep_size = mesh.shape["ep"]

    def local_block(hidden_in, norm_gain, router_w, w_gate, w_up, w_down, ws_gate, ws_up, ws_down, expert_ids):
        tok, top_k = expert_ids.shape
        dim = hidden_in.shape[1]
        n_exp, _, inter = w_gate.shape
        s_inter = ws_gate.shape[1]
        cap = GROUPS * ((top_k + GROUP_LIMIT - 1) // GROUP_LIMIT) * tok // n_exp
        rows = ep_size * tok
        pairs = n_exp * cap
        n_blk = dim // COLS
        chips = ep_size // CORES
        vm = pltpu.VMEM
        n_remote = 6 + 7 + (ep_size - 1) + 7 * n_blk
        scratch = [
            vm((tok, dim), BF16), vm((1, dim), F32), vm(router_w.shape, F32), vm((top_k, tok), jnp.int32),
            vm(w_gate.shape, BF16), vm(w_up.shape, BF16), vm(w_down.shape, BF16),
            vm(ws_gate.shape, BF16), vm(ws_up.shape, BF16), vm(ws_down.shape, BF16),
            vm((ep_size, tok, dim), BF16), vm((ep_size, n_exp, 128), F32), vm((ep_size, n_exp, 128), F32),
            vm((pairs, rows), BF16), vm((pairs, rows), F32),
            vm((rows, pairs), BF16), vm((rows, pairs), BF16), vm((rows, pairs), BF16),
            vm((pairs, dim), BF16), vm((pairs, inter), BF16), vm((pairs, COLS), BF16),
            vm((n_blk, CORES, chips * tok, COLS), F32), vm((n_blk, chips * tok, COLS), F32), vm((n_blk, chips, tok, COLS), F32),
            vm((n_blk, tok, COLS // 2), F32), vm((n_blk, tok, COLS // 2), F32), vm((n_blk, tok, COLS // 2), F32), vm((n_blk, tok, COLS // 2), F32),
            vm((n_blk, tok, COLS), F32), vm((n_blk, tok, COLS), F32),
            vm((tok, s_inter), BF16), vm((tok, dim), BF16),
            pltpu.SemaphoreType.DMA((4,)), pltpu.SemaphoreType.DMA((3 * n_exp + 3,)),
            pltpu.SemaphoreType.DMA((n_remote,)), pltpu.SemaphoreType.DMA((n_remote,)),
        ]
        return pl.pallas_call(
            functools.partial(moe_kernel, ep_size, cap),
            out_shape=jax.ShapeDtypeStruct((tok, dim), BF16),
            in_specs=[pl.BlockSpec(memory_space=pl.ANY)] * 10,
            out_specs=pl.BlockSpec(memory_space=pltpu.VMEM),
            scratch_shapes=scratch,
            compiler_params=pltpu.CompilerParams(collective_id=0, has_side_effects=True, vmem_limit_bytes=67_000_000),
            name="moe_block",
        )(hidden_in, norm_gain[None, :], router_w, w_gate, w_up, w_down, ws_gate, ws_up, ws_down, expert_ids.T)

    row_spec = P(("dp", "ep"), None)
    in_specs = (row_spec, P(), P(), P("ep"), P("ep"), P("ep"), P(), P(), P(), row_spec)
    return jax.shard_map(local_block, mesh=mesh, in_specs=in_specs, out_specs=row_spec, check_vma=False)
```

```python
import functools

import jax
import jax.numpy as jnp
from jax import lax
from jax.experimental import pallas as pl
from jax.experimental.pallas import tpu as pltpu
from jax.sharding import PartitionSpec as P

NORM_EPS = 1e-6
ROUTE_SCALE = 2.5
GROUPS = 8
GROUP_LIMIT = 4
CORES = 2
COLS = 256
MESH = pl.DeviceIdType.MESH
F32 = jnp.float32
BF16 = jnp.bfloat16


def dot(a, b):
    return jnp.dot(a, b, preferred_element_type=F32)


def dot_t(a, b):
    return lax.dot_general(a, b, (((1,), (1,)), ((), ())), preferred_element_type=F32)


def split3(v):
    hi = v.astype(BF16)
    rest = v - hi.astype(F32)
    mid = rest.astype(BF16)
    low = (rest - mid.astype(F32)).astype(BF16)
    return hi, mid, low


def moe_kernel(ep_size, cap, hid_h, gain_h, rw_h, wg_h, wu_h, wd_h, sg_h, su_h, sd_h, ids_h, out_ref,
               hid, gain, rw, ids, wg, wu, wd, sg, su, sd, x_all, gt_send, gt_all, p_all, ga, acat,
               xg, hbuf, ybuf, sbuf, d2d, tbuf, hop, rel, froml, fromr, hsh, shared,
               obuf, in_sem, w_sem, o_sem,
               ring_s, cross_s, tile_s, d2d_s, hop_s, dir_s, rel_s, ag_r, cross_r, tile_r, d2d_r, hop_r, end_r):
    chips = ep_size // CORES
    tok, dim = hid.shape
    n_exp, _, inter = wg.shape
    top_k = ids.shape[0]
    half = dim // 2
    rows = ep_size * tok
    n_blk = dim // COLS
    hc = COLS // 2
    pairs = n_exp * cap

    me = lax.axis_index("ep")
    chip, core = me // CORES, me % CORES
    other = 1 - core
    right, left, opp = (chip + 1) % chips, (chip + chips - 1) % chips, (chip + 2) % chips

    def slot(a_chip, a_core):
        return a_core * chips + a_chip

    def dev(a_chip, a_core):
        return {"ep": a_chip * CORES + a_core}

    def remote(src, dst, to, s_sem, r_sem):
        copy = pltpu.make_async_remote_copy(src, dst, s_sem, r_sem, device_id=to, device_id_type=MESH)
        copy.start()
        return copy

    def await_all(ref, sem):
        pltpu.make_async_copy(ref, ref, sem).wait()

    ins = [pltpu.make_async_copy(s, d, in_sem.at[i]) for i, (s, d) in enumerate(((hid_h, hid), (gain_h, gain), (rw_h, rw), (ids_h, ids)))]
    for copy in ins:
        copy.start()
    weights = []
    for i, (s, d) in enumerate(((wg_h, wg), (wu_h, wu), (wd_h, wd), (sg_h, sg), (su_h, su), (sd_h, sd))):
        weights.append(pltpu.make_async_copy(s, d, w_sem.at[i]))
        weights[-1].start(priority=1)

    barrier = pltpu.get_barrier_semaphore()
    for k in range(1, ep_size):
        pl.semaphore_signal(barrier, inc=1, device_id={"ep": (me + k) % ep_size}, device_id_type=MESH)

    mine = slot(chip, core)
    with jax.named_scope("norm"):
        ins[0].wait()
        ins[1].wait()
        x_f32 = hid[...].astype(F32)
        inv_rms = lax.rsqrt(jnp.mean(x_f32 * x_f32, axis=-1, keepdims=True) + NORM_EPS)
        gain_row = jnp.concatenate([gain[i : i + 1, :] for i in range(dim // 128)], axis=1)
        x_norm = (x_f32 * inv_rms * gain_row).astype(BF16)
        x_all[mine] = x_norm

    with jax.named_scope("barwait"):
        pl.semaphore_wait(barrier, ep_size - 1)

    quarter = half // 2
    q = [slice(k * quarter, (k + 1) * quarter) for k in range(4)]
    part_a, part_b = slice(0, half), slice(half, dim)

    def spread(a_slot, cols, to, r_sem):
        ref = x_all.at[a_slot, :, cols]
        return remote(ref, ref, to, ring_s, r_sem)

    def cross(a_slot, cols):
        ref = x_all.at[a_slot, :, cols]
        remote(ref, ref, dev(chip, other), cross_s, cross_r)

    ra = [spread(mine, q[k], dev(right, core), ag_r.at[k]) for k in range(2)]
    lb = [spread(mine, q[2 + k], dev(left, core), ag_r.at[2 + k]) for k in range(2)]
    rb = spread(mine, part_b, dev(right, core), ag_r.at[4])
    la = spread(mine, part_a, dev(left, core), ag_r.at[5])
    cross(mine, slice(0, dim))

    with jax.named_scope("router"):
        ins[2].wait()
        ins[3].wait()
        r_hi, r_mid, r_low = split3(rw[...])
        logits = (dot_t(r_low, x_norm) + dot_t(r_mid, x_norm)) + dot_t(r_hi, x_norm)
        scores = 1.0 / (1.0 + jnp.exp(-logits))
        exp_no = lax.broadcasted_iota(jnp.int32, logits.shape, 0)
        chosen = exp_no == ids[0:1, :]
        for k in range(1, top_k):
            chosen = jnp.logical_or(chosen, exp_no == ids[k : k + 1, :])
        total = jnp.sum(jnp.where(chosen, scores, 0.0), axis=0, keepdims=True)
        gates = jnp.where(chosen, ROUTE_SCALE * scores / total, -1.0)
        gt_send[...] = jnp.full(gt_send.shape, -1.0, F32)
        for d in range(ep_size):
            gt_send[d, :, 0:tok] = gates[d * n_exp : (d + 1) * n_exp, :]
        gt_all[mine] = gt_send[me]
        for k in range(1, ep_size):
            to = (me + k) % ep_size
            remote(gt_send.at[to], gt_all.at[mine], {"ep": to}, tile_s, tile_r)

    with jax.named_scope("relays"):
        for k in range(2):
            ra[k].wait_recv()
            spread(slot(left, core), q[k], dev(right, core), ag_r.at[6])
            cross(slot(left, core), q[k])
            lb[k].wait_recv()
            spread(slot(right, core), q[2 + k], dev(left, core), ag_r.at[7])
            cross(slot(right, core), q[2 + k])
        rb.wait_recv()
        cross(slot(left, core), part_b)
        la.wait_recv()
        cross(slot(right, core), part_a)

    with jax.named_scope("tilewait"):
        await_all(gt_all.at[0 : ep_size - 1], tile_r)

    with jax.named_scope("onehot"):
        lane_src = lax.broadcasted_iota(jnp.int32, (n_exp, rows), 1) // tok
        gmat = jnp.full((n_exp, rows), -1.0, F32)
        for s in range(ep_size):
            wide = jnp.concatenate([gt_all[s], jnp.full((n_exp, rows - gt_all.shape[2]), -1.0, F32)], axis=1)
            if s:
                wide = pltpu.roll(wide, s * tok, 1)
            gmat = jnp.where(lane_src == s, wide, gmat)
        picked = jnp.logical_not(gmat < 0.0)
        upper = lax.broadcasted_iota(jnp.int32, (rows, rows), 0) < lax.broadcasted_iota(jnp.int32, (rows, rows), 1)
        rank = dot(jnp.where(picked, 1.0, 0.0).astype(BF16), jnp.where(upper, 1.0, 0.0).astype(BF16))
        place = jnp.where(picked, rank, -1.0)
        row_no = lax.broadcasted_iota(jnp.int32, (cap, rows), 0).astype(F32)
        for e in range(n_exp):
            hit = row_no == place[e : e + 1, :]
            p_all[e * cap : (e + 1) * cap, :] = jnp.where(hit, 1.0, 0.0).astype(BF16)
            ga[e * cap : (e + 1) * cap, :] = jnp.where(hit, gmat[e : e + 1, :], 0.0)
        for i in range(n_exp * cap // 128):
            lanes = slice(i * 128, (i + 1) * 128)
            hi, mid, low = split3(ga[lanes, :].T)
            for k, term in enumerate((low, mid, hi)):
                acat[:, k * pairs + i * 128 : k * pairs + (i + 1) * 128] = term

    with jax.named_scope("agwait"):
        await_all(x_all.at[slot(opp, core), :, part_a], ag_r.at[6])
        cross(slot(opp, core), part_a)
        await_all(x_all.at[slot(opp, core), :, part_b], ag_r.at[7])
        cross(slot(opp, core), part_b)
        await_all(x_all.at[pl.ds(other * chips, chips)], cross_r)

    with jax.named_scope("wwait"):
        weights[0].wait()
        weights[1].wait()

    with jax.named_scope("gateup"):
        x_rows = x_all[...].reshape(rows, dim)

        def gather(e):
            xg[(e // 2) % 2] = dot(p_all[e * cap : (e + 2) * cap, :], x_rows).astype(BF16)

        gather(0)
        for e in range(n_exp):
            if e % 2 == 0 and e + 2 < n_exp:
                gather(e + 2)
            xe = xg[(e // 2) % 2, (e % 2) * cap : (e % 2 + 1) * cap, :]
            h_gate = dot(xe, wg[e])
            h_up = dot(xe, wu[e])
            hbuf[e * cap : (e + 1) * cap, :] = (jax.nn.silu(h_gate) * h_up).astype(BF16)

    with jax.named_scope("dwait"):
        weights[2].wait()

    part = []

    def last(j):
        cols = slice(j * COLS, (j + 1) * COLS)
        for e in range(n_exp):
            y = dot(hbuf[e * cap : (e + 1) * cap, :], wd[e, :, cols]).astype(BF16)
            for k in range(3):
                ybuf[j % 2, k * pairs + e * cap : k * pairs + (e + 1) * cap, :] = y

    def compute(j):
        if j == 1:
            last(1)
        if j and j + 1 < n_blk:
            last(j + 1)
        for k in range(CORES):
            sbuf[j, k] = dot(acat[k * chips * tok : (k + 1) * chips * tok, :], ybuf[j % 2])
        part.append(remote(sbuf.at[j, other], d2d.at[j], dev(chip, other), d2d_s, d2d_r.at[j]))

    lo, up = slice(0, hc), slice(hc, COLS)
    half_blk = n_blk // 2

    def send(j):
        part[j].wait_recv()
        tbuf[j] = (sbuf[j, core] + d2d[j]).reshape(chips, tok, COLS)
        remote(tbuf.at[j, opp, :, lo], hop.at[j, :, lo], dev(right, core), hop_s, hop_r.at[j])
        remote(tbuf.at[j, opp, :, up], hop.at[j, :, up], dev(left, core), hop_s, hop_r.at[j])

    def direct(j):
        remote(tbuf.at[j, right, :, up], froml.at[j, :, up], dev(right, core), dir_s, end_r.at[0, j // half_blk])
        remote(tbuf.at[j, left, :, lo], fromr.at[j, :, lo], dev(left, core), dir_s, end_r.at[1, j // half_blk])

    def relay(j):
        await_all(hop.at[j], hop_r.at[j])
        rel[j, :, lo] = hop[j, :, lo] + tbuf[j, right, :, lo]
        rel[j, :, up] = hop[j, :, up] + tbuf[j, left, :, up]
        remote(rel.at[j, :, lo], froml.at[j, :, lo], dev(right, core), rel_s, end_r.at[0, j // half_blk])
        remote(rel.at[j, :, up], fromr.at[j, :, up], dev(left, core), rel_s, end_r.at[1, j // half_blk])

    def finish(k):
        blks = slice(k * half_blk, (k + 1) * half_blk)
        await_all(froml.at[blks], end_r.at[0, k])
        await_all(fromr.at[blks], end_r.at[1, k])
        for j in range(k * half_blk, (k + 1) * half_blk):
            cols = slice(j * COLS, (j + 1) * COLS)
            routed = (tbuf[j, chip] + froml[j]) + fromr[j]
            obuf[:, cols] = ((hid[:, cols].astype(F32) + shared[:, cols].astype(F32)) + routed).astype(BF16)
        cols = slice(k * half_blk * COLS, (k + 1) * half_blk * COLS)
        pltpu.make_async_copy(obuf.at[:, cols], out_ref.at[:, cols], o_sem).start()

    def scoped(f, j):
        with jax.named_scope(f"{f.__name__}{j}"):
            f(j)

    last(0)
    for j in range(n_blk):
        scoped(compute, j)
        if j >= 1:
            scoped(send, j - 1)
            scoped(direct, j - 1)
    scoped(send, n_blk - 1)

    with jax.named_scope("shared"):
        for copy in weights[3:]:
            copy.wait()
        xs = x_all[mine]
        mid_cols = hsh.shape[1] // 2

        def shared_part(k):
            cols = slice(k * mid_cols, (k + 1) * mid_cols)
            hsh[:, cols] = (jax.nn.silu(dot(xs, sg[:, cols])) * dot(xs, su[:, cols])).astype(BF16)

        scoped(relay, 0)
        scoped(relay, 1)
        scoped(direct, n_blk - 1)
        shared_part(0)
        scoped(relay, 2)
        scoped(relay, 3)
        shared_part(1)
        scoped(relay, 4)
        scoped(relay, 5)
        shared[...] = dot(hsh[...], sd[...]).astype(BF16)
    for k in range(2):
        scoped(finish, k)
    with jax.named_scope("drain"):
        await_all(x_all.at[0:3], ring_s)
        await_all(x_all.at[0:chips], cross_s)
        await_all(gt_send.at[0 : ep_size - 1], tile_s)
        await_all(d2d, d2d_s)
        await_all(hop, hop_s)
        await_all(froml, dir_s)
        await_all(rel, rel_s)
        pltpu.make_async_copy(obuf, out_ref, o_sem).wait()


def solution(mesh):
    ep_size = mesh.shape["ep"]

    def local_block(hidden_in, norm_gain, router_w, w_gate, w_up, w_down, ws_gate, ws_up, ws_down, expert_ids):
        tok, top_k = expert_ids.shape
        dim = hidden_in.shape[1]
        n_exp, _, inter = w_gate.shape
        s_inter = ws_gate.shape[1]
        cap = GROUPS * ((top_k + GROUP_LIMIT - 1) // GROUP_LIMIT) * tok // n_exp
        rows = ep_size * tok
        pairs = n_exp * cap
        n_blk = dim // COLS
        chips = ep_size // CORES
        vm, sem = pltpu.VMEM, pltpu.SemaphoreType.DMA
        scratch = [
            vm((tok, dim), BF16), vm((dim // 128, 128), F32), vm(router_w.shape, F32), vm((top_k, tok), jnp.int32),
            vm(w_gate.shape, BF16), vm(w_up.shape, BF16), vm(w_down.shape, BF16),
            vm(ws_gate.shape, BF16), vm(ws_up.shape, BF16), vm(ws_down.shape, BF16),
            vm((ep_size, tok, dim), BF16), vm((ep_size, n_exp, 128), F32), vm((ep_size, n_exp, 128), F32),
            vm((pairs, rows), BF16), vm((pairs, rows), F32),
            vm((rows, 3 * pairs), BF16),
            vm((2, 2 * cap, dim), BF16), vm((pairs, inter), BF16), vm((2, 3 * pairs, COLS), BF16),
            vm((n_blk, CORES, chips * tok, COLS), F32), vm((n_blk, chips * tok, COLS), F32), vm((n_blk, chips, tok, COLS), F32),
            vm((n_blk, tok, COLS), F32), vm((n_blk, tok, COLS), F32), vm((n_blk, tok, COLS), F32), vm((n_blk, tok, COLS), F32),
            vm((tok, s_inter), BF16), vm((tok, dim), BF16), vm((tok, dim), BF16),
            sem((4,)), sem((6,)), sem, sem, sem, sem, sem, sem, sem, sem,
            sem((8,)), sem, sem, sem((n_blk,)), sem((n_blk,)), sem((2, 2)),
        ]
        return pl.pallas_call(
            functools.partial(moe_kernel, ep_size, cap),
            out_shape=jax.ShapeDtypeStruct((tok, dim), BF16),
            in_specs=[pl.BlockSpec(memory_space=pl.ANY)] * 10,
            out_specs=pl.BlockSpec(memory_space=pl.ANY),
            scratch_shapes=scratch,
            compiler_params=pltpu.CompilerParams(collective_id=0, has_side_effects=True, vmem_limit_bytes=67_000_000),
            name="moe_block",
        )(hidden_in, norm_gain.reshape(dim // 128, 128), router_w, w_gate, w_up, w_down, ws_gate, ws_up, ws_down, expert_ids.T)

    row_spec = P(("dp", "ep"), None)
    in_specs = (row_spec, P(), P(), P("ep"), P("ep"), P("ep"), P(), P(), P(), row_spec)
    return jax.shard_map(local_block, mesh=mesh, in_specs=in_specs, out_specs=row_spec, check_vma=False)
```

```python
import functools

import jax
import jax.numpy as jnp
from jax import lax
from jax.experimental import pallas as pl
from jax.experimental.pallas import tpu as pltpu
from jax.sharding import PartitionSpec as P

NORM_EPS = 1e-6
ROUTE_SCALE = 2.5
GROUPS = 8
GROUP_LIMIT = 4
CORES = 2
POS_OWN, POS_RIGHT, POS_LEFT, POS_FAR = range(4)
COLS = 256
MESH = pl.DeviceIdType.MESH
F32 = jnp.float32
BF16 = jnp.bfloat16


def dot(a, b):
    return jnp.dot(a, b, preferred_element_type=F32)


def dot_t(a, b):
    return lax.dot_general(a, b, (((1,), (1,)), ((), ())), preferred_element_type=F32)


def split3(v):
    hi = v.astype(BF16)
    rest = v - hi.astype(F32)
    mid = rest.astype(BF16)
    low = (rest - mid.astype(F32)).astype(BF16)
    return hi, mid, low


def moe_kernel(ep_size, cap, hid_h, gain_h, rw_h, wg_h, wu_h, wd_h, sg_h, su_h, sd_h, ids_h, out_ref,
               hid, gain, rw, ids, wg, wu, wd, sg, su, sd, x_all, gt_send, gt_all, p_all, acat,
               xg, hbuf, ybuf, sbuf, d2d, tbuf, hop, rel, froml, fromr, hsh, shared,
               in_sem, w_sem,
               ring_s, cross_s, tile_s, d2d_s, hop_s, dir_s, rel_s, ag_r, cross_r, tile_r, d2d_r, hop_r, end_r):
    chips = ep_size // CORES
    tok, dim = hid.shape
    n_exp, _, inter = wg.shape
    top_k = ids.shape[0]
    half = dim // 2
    rows = ep_size * tok
    n_blk = dim // COLS
    hc = COLS // 2
    pairs = n_exp * cap

    me = lax.axis_index("ep")
    chip, core = me // CORES, me % CORES
    other = 1 - core
    right, left, opp = (chip + 1) % chips, (chip + chips - 1) % chips, (chip + 2) % chips

    def slot(a_chip, a_core, at=None):
        away = (a_chip - (chip if at is None else at) + chips) % chips
        return (away + away // 2 - 2 * (away // 3)) * CORES + a_core

    def dev(a_chip, a_core):
        return {"ep": a_chip * CORES + a_core}

    def remote(src, dst, to, s_sem, r_sem):
        copy = pltpu.make_async_remote_copy(src, dst, s_sem, r_sem, device_id=to, device_id_type=MESH)
        copy.start()
        return copy

    def await_all(ref, sem):
        pltpu.make_async_copy(ref, ref, sem).wait()

    ins = [pltpu.make_async_copy(s, d, in_sem.at[i]) for i, (s, d) in enumerate(((hid_h, hid), (gain_h, gain), (rw_h, rw), (ids_h, ids)))]
    for copy in ins:
        copy.start()
    early, late = slice(0, COLS), slice(COLS, dim)
    fetches = ((wg_h, wg), (wu_h, wu), (wd_h.at[:, :, early], wd.at[:, :, early]), (wd_h.at[:, :, late], wd.at[:, :, late]), (sg_h, sg), (su_h, su), (sd_h, sd))
    weights = []
    for i, (s, d) in enumerate(fetches):
        weights.append(pltpu.make_async_copy(s, d, w_sem.at[i]))
        weights[-1].start(priority=1)

    barrier = pltpu.get_barrier_semaphore()
    for k in range(1, ep_size):
        pl.semaphore_signal(barrier, inc=1, device_id={"ep": (me + k) % ep_size}, device_id_type=MESH)

    mine = slot(chip, core)
    with jax.named_scope("norm"):
        ins[0].wait()
        ins[1].wait()
        x_f32 = hid[...].astype(F32)
        inv_rms = lax.rsqrt(jnp.mean(x_f32 * x_f32, axis=-1, keepdims=True) + NORM_EPS)
        gain_row = jnp.concatenate([gain[i : i + 1, :] for i in range(dim // 128)], axis=1)
        x_norm = (x_f32 * inv_rms * gain_row).astype(BF16)
        x_all[mine] = x_norm

    with jax.named_scope("barwait"):
        pl.semaphore_wait(barrier, ep_size - 1)

    half = dim // 2
    q = [slice(k * half // 2, (k + 1) * half // 2) for k in range(4)]
    part_a, part_b = slice(0, half), slice(half, dim)

    def spread(a_chip, cols, to, r_sem):
        src, dst = x_all.at[slot(a_chip, core), :, cols], x_all.at[slot(a_chip, core, to), :, cols]
        return remote(src, dst, dev(to, core), ring_s, r_sem)

    def cross(a_chip, cols, r_sem):
        ref = x_all.at[slot(a_chip, core), :, cols]
        remote(ref, ref, dev(chip, other), cross_s, r_sem)

    ra, lb = [], []
    for k in range(2):
        ra.append(spread(chip, q[k], right, ag_r.at[k]))
        lb.append(spread(chip, q[2 + k], left, ag_r.at[2 + k]))

    with jax.named_scope("router"):
        ins[2].wait()
        ins[3].wait()
        r_hi, r_mid, r_low = split3(rw[...])
        logits = (dot_t(r_low, x_norm) + dot_t(r_mid, x_norm)) + dot_t(r_hi, x_norm)
        scores = 1.0 / (1.0 + jnp.exp(-logits))
        exp_no = lax.broadcasted_iota(jnp.int32, logits.shape, 0)
        chosen = exp_no == ids[0:1, :]
        for k in range(1, top_k):
            chosen = jnp.logical_or(chosen, exp_no == ids[k : k + 1, :])
        total = jnp.sum(jnp.where(chosen, scores, 0.0), axis=0, keepdims=True)
        gates = jnp.where(chosen, ROUTE_SCALE * scores / total, -1.0)
        gt_send[...] = jnp.full(gt_send.shape, -1.0, F32)
        for d in range(ep_size):
            gt_send[d, :, 0:tok] = gates[d * n_exp : (d + 1) * n_exp, :]
        gt_all[mine] = gt_send[me]
        for k in range(1, ep_size):
            to = (me + k) % ep_size
            remote(gt_send.at[to], gt_all.at[slot(chip, core, to // CORES)], {"ep": to}, tile_s, tile_r)

    rb = spread(chip, part_b, right, ag_r.at[4])
    la = spread(chip, part_a, left, ag_r.at[5])
    cross(chip, slice(0, dim), cross_r.at[0])

    with jax.named_scope("relays"):
        for k in range(2):
            ra[k].wait_recv()
            spread(left, q[k], right, ag_r.at[6])
            cross(left, q[k], cross_r.at[0])
            lb[k].wait_recv()
            spread(right, q[2 + k], left, ag_r.at[7])
            cross(right, q[2 + k], cross_r.at[0])

    def near_rest():
        rb.wait_recv()
        cross(left, part_b, cross_r.at[0])
        la.wait_recv()
        cross(right, part_a, cross_r.at[0])

    with jax.named_scope("tilewait"):
        await_all(gt_all.at[0 : ep_size - 1], tile_r)

    with jax.named_scope("onehot"):
        lane_src = lax.broadcasted_iota(jnp.int32, (n_exp, rows), 1) // tok
        gmat = jnp.full((n_exp, rows), -1.0, F32)
        for s in range(ep_size):
            wide = jnp.concatenate([gt_all[s], jnp.full((n_exp, rows - gt_all.shape[2]), -1.0, F32)], axis=1)
            if s:
                wide = pltpu.roll(wide, s * tok, 1)
            gmat = jnp.where(lane_src == s, wide, gmat)
        picked = jnp.logical_not(gmat < 0.0)
        upper = lax.broadcasted_iota(jnp.int32, (rows, rows), 0) < lax.broadcasted_iota(jnp.int32, (rows, rows), 1)
        rank = dot(jnp.where(picked, 1.0, 0.0).astype(BF16), jnp.where(upper, 1.0, 0.0).astype(BF16))
        place = jnp.where(picked, rank, -1.0)
        for i in range(pairs // 128):
            e_one, e_two = i * 128 // cap, (i * 128 + 127) // cap
            row_no = lax.broadcasted_iota(jnp.int32, (128, rows), 0) + i * 128
            first = row_no < e_two * cap
            pos = (row_no - jnp.where(first, e_one * cap, e_two * cap)).astype(F32)
            hit = pos == jnp.where(first, place[e_one : e_one + 1, :], place[e_two : e_two + 1, :])
            gated = jnp.where(hit, jnp.where(first, gmat[e_one : e_one + 1, :], gmat[e_two : e_two + 1, :]), 0.0)
            p_all[i * 128 : (i + 1) * 128, :] = jnp.where(hit, 1.0, 0.0).astype(BF16)
            for k, term in enumerate(reversed(split3(gated.T))):
                for b in range(ep_size):
                    to_row = ((b % CORES) * chips + b // CORES) * tok
                    acat[to_row : to_row + tok, k * pairs + i * 128 : k * pairs + (i + 1) * 128] = term[b * tok : (b + 1) * tok, :]

    n_near = rows - CORES * tok
    stack = pairs // 4

    def gather_near(k):
        at = slice(k * stack, (k + 1) * stack)
        xg[at, :] = dot(p_all[at, 0:n_near], x_all[0 : ep_size - CORES].reshape(n_near, dim)).astype(BF16)

    with jax.named_scope("nearrest"):
        near_rest()
    with jax.named_scope("nearwait"):
        await_all(x_all.at[0 : chips - 1], cross_r.at[0])
    with jax.named_scope("near0"):
        gather_near(0)
    with jax.named_scope("far"):
        await_all(x_all.at[mine, :, part_a], ag_r.at[6])
        cross(opp, part_a, cross_r.at[1])
        await_all(x_all.at[mine, :, part_b], ag_r.at[7])
        cross(opp, part_b, cross_r.at[1])
    with jax.named_scope("near1"):
        for k in range(1, 4):
            gather_near(k)
    with jax.named_scope("farwait"):
        await_all(x_all.at[mine], cross_r.at[1])
        for copy in weights[:3]:
            copy.wait()

    part = []

    def last(j):
        cols = slice(j * COLS, (j + 1) * COLS)
        for e in range(n_exp):
            y = dot(hbuf[e * cap : (e + 1) * cap, :], wd[e, :, cols]).astype(BF16)
            for k in range(3):
                ybuf[j % 2, k * pairs + e * cap : k * pairs + (e + 1) * cap, :] = y

    def compute(j):
        if j == 1:
            last(1)
        if j and j + 1 < n_blk:
            last(j + 1)
        for k in range(CORES):
            sbuf[j, k] = dot(acat[k * chips * tok : (k + 1) * chips * tok, :], ybuf[j % 2])
        part.append(remote(sbuf.at[j, other], d2d.at[j], dev(chip, other), d2d_s, d2d_r.at[j]))

    lo, up = slice(0, hc), slice(hc, COLS)
    half_blk = n_blk // 2

    def send(j):
        part[j].wait_recv()
        tbuf[j] = (sbuf[j, core] + d2d[j]).reshape(chips, tok, COLS)
        remote(tbuf.at[j, POS_FAR, :, lo], hop.at[j, :, lo], dev(right, core), hop_s, hop_r.at[j])
        remote(tbuf.at[j, POS_FAR, :, up], hop.at[j, :, up], dev(left, core), hop_s, hop_r.at[j])

    def direct(j):
        remote(tbuf.at[j, POS_RIGHT, :, up], froml.at[j, :, up], dev(right, core), dir_s, end_r.at[0, j // half_blk])
        remote(tbuf.at[j, POS_LEFT, :, lo], fromr.at[j, :, lo], dev(left, core), dir_s, end_r.at[1, j // half_blk])

    def relay(j):
        await_all(hop.at[j], hop_r.at[j])
        rel[j, :, lo] = hop[j, :, lo] + tbuf[j, POS_RIGHT, :, lo]
        rel[j, :, up] = hop[j, :, up] + tbuf[j, POS_LEFT, :, up]
        remote(rel.at[j, :, lo], froml.at[j, :, lo], dev(right, core), rel_s, end_r.at[0, j // half_blk])
        remote(rel.at[j, :, up], fromr.at[j, :, up], dev(left, core), rel_s, end_r.at[1, j // half_blk])

    def finish(k):
        blks = slice(k * half_blk, (k + 1) * half_blk)
        await_all(froml.at[blks], end_r.at[0, k])
        await_all(fromr.at[blks], end_r.at[1, k])
        for j in range(k * half_blk, (k + 1) * half_blk):
            cols = slice(j * COLS, (j + 1) * COLS)
            routed = (tbuf[j, POS_OWN] + froml[j]) + fromr[j]
            out_ref[:, cols] = ((hid[:, cols].astype(F32) + shared[:, cols].astype(F32)) + routed).astype(BF16)

    def scoped(f, j):
        with jax.named_scope(f"{f.__name__}{j}"):
            f(j)

    with jax.named_scope("gateup"):
        x_far = x_all[ep_size - CORES : ep_size].reshape(CORES * tok, dim)
        for e in range(n_exp):
            if e % 2 == 0:
                two = slice(e * cap, (e + 2) * cap)
                xg[two, :] = xg[two, :] + dot(p_all[two, n_near:], x_far).astype(BF16)
            own = slice(e * cap, (e + 1) * cap)
            h_gate = dot(xg[own, :], wg[e])
            h_up = dot(xg[own, :], wu[e])
            hbuf[own, :] = (jax.nn.silu(h_gate) * h_up).astype(BF16)
        last(0)
        compute(0)
    weights[3].wait()
    for j in range(n_blk):
        if j:
            scoped(compute, j)
        if j >= 1:
            scoped(send, j - 1)
            scoped(direct, j - 1)
    scoped(send, n_blk - 1)

    with jax.named_scope("shared"):
        for copy in weights[4:]:
            copy.wait()
        xs = x_all[mine]
        mid_cols = hsh.shape[1] // 2

        def shared_part(k):
            cols = slice(k * mid_cols, (k + 1) * mid_cols)
            hsh[:, cols] = (jax.nn.silu(dot(xs, sg[:, cols])) * dot(xs, su[:, cols])).astype(BF16)

        scoped(relay, 0)
        scoped(relay, 1)
        scoped(direct, n_blk - 1)
        shared_part(0)
        scoped(relay, 2)
        scoped(relay, 3)
        shared_part(1)
        scoped(relay, 4)
        scoped(relay, 5)
        shared[...] = dot(hsh[...], sd[...]).astype(BF16)
    for k in range(2):
        scoped(finish, k)
    with jax.named_scope("drain"):
        await_all(x_all.at[0:3], ring_s)
        await_all(x_all.at[0:chips], cross_s)
        await_all(gt_send.at[0 : ep_size - 1], tile_s)
        await_all(d2d, d2d_s)
        await_all(hop, hop_s)
        await_all(froml, dir_s)
        await_all(rel, rel_s)


def put_kernel(src, dst, o_sem):
    copy = pltpu.make_async_copy(src, dst, o_sem)
    copy.start()
    copy.wait()


def solution(mesh):
    ep_size = mesh.shape["ep"]

    def local_block(hidden_in, norm_gain, router_w, w_gate, w_up, w_down, ws_gate, ws_up, ws_down, expert_ids):
        tok, top_k = expert_ids.shape
        dim = hidden_in.shape[1]
        n_exp, _, inter = w_gate.shape
        s_inter = ws_gate.shape[1]
        cap = GROUPS * ((top_k + GROUP_LIMIT - 1) // GROUP_LIMIT) * tok // n_exp
        rows = ep_size * tok
        pairs = n_exp * cap
        n_blk = dim // COLS
        chips = ep_size // CORES
        vm, sem = pltpu.VMEM, pltpu.SemaphoreType.DMA
        scratch = [
            vm((tok, dim), BF16), vm((dim // 128, 128), F32), vm(router_w.shape, F32), vm((top_k, tok), jnp.int32),
            vm(w_gate.shape, BF16), vm(w_up.shape, BF16), vm(w_down.shape, BF16),
            vm(ws_gate.shape, BF16), vm(ws_up.shape, BF16), vm(ws_down.shape, BF16),
            vm((ep_size, tok, dim), BF16), vm((ep_size, n_exp, 128), F32), vm((ep_size, n_exp, 128), F32),
            vm((pairs, rows), BF16),
            vm((rows, 3 * pairs), BF16),
            vm((pairs, dim), BF16), vm((pairs, inter), BF16), vm((2, 3 * pairs, COLS), BF16),
            vm((n_blk, CORES, chips * tok, COLS), F32), vm((n_blk, chips * tok, COLS), F32), vm((n_blk, chips, tok, COLS), F32),
            vm((n_blk, tok, COLS), F32), vm((n_blk, tok, COLS), F32), vm((n_blk, tok, COLS), F32), vm((n_blk, tok, COLS), F32),
            vm((tok, s_inter), BF16), vm((tok, dim), BF16),
            sem((4,)), sem((7,)), sem, sem, sem, sem, sem, sem, sem,
            sem((8,)), sem((2,)), sem, sem((n_blk,)), sem((n_blk,)), sem((2, 2)),
        ]
        result = pl.pallas_call(
            functools.partial(moe_kernel, ep_size, cap),
            out_shape=pltpu.VMEM((tok, dim), BF16),
            in_specs=[pl.BlockSpec(memory_space=pl.ANY)] * 10,
            out_specs=pl.BlockSpec(memory_space=pltpu.VMEM),
            scratch_shapes=scratch,
            compiler_params=pltpu.CompilerParams(collective_id=0, has_side_effects=True, vmem_limit_bytes=64_900_000),
            name="moe_block",
        )(hidden_in, norm_gain.reshape(dim // 128, 128), router_w, w_gate, w_up, w_down, ws_gate, ws_up, ws_down, expert_ids.T)
        return result

    row_spec = P(("dp", "ep"), None)
    in_specs = (row_spec, P(), P(), P("ep"), P("ep"), P("ep"), P(), P(), P(), row_spec)
    return jax.shard_map(local_block, mesh=mesh, in_specs=in_specs, out_specs=row_spec, check_vma=False)
```

```python
import functools

import jax
import jax.numpy as jnp
from jax import lax
from jax.experimental import pallas as pl
from jax.experimental.pallas import tpu as pltpu
from jax.sharding import PartitionSpec as P

NORM_EPS = 1e-6
ROUTE_SCALE = 2.5
GROUPS = 8
GROUP_LIMIT = 4
CORES = 2
S_ROW = (0, 1, 2, 4, 5, 6, 3, 7)
POS_OWN, POS_RIGHT, POS_LEFT, POS_FAR = range(4)
COLS = 256
MESH = pl.DeviceIdType.MESH
F32 = jnp.float32
BF16 = jnp.bfloat16


def dot(a, b):
    return jnp.dot(a, b, preferred_element_type=F32)


def dot_t(a, b):
    return lax.dot_general(a, b, (((1,), (1,)), ((), ())), preferred_element_type=F32)


def split3(v):
    hi = v.astype(BF16)
    rest = v - hi.astype(F32)
    mid = rest.astype(BF16)
    low = (rest - mid.astype(F32)).astype(BF16)
    return hi, mid, low


def moe_kernel(ep_size, cap, hid_h, gain_h, rw_h, wg_h, wu_h, wd_h, sg_h, su_h, sd_h, ids_h, out_ref,
               hid, gain, rw, ids, wg, wu, wd, sg, su, sd, x_all, gt_send, gt_all, p_all, acat,
               xg, hbuf, ybuf, sbuf, d2d, tbuf, hop, rel, froml, fromr, hsh, shared,
               in_sem, w_sem,
               ring_s, cross_s, tile_s, d2d_s, hop_s, dir_s, rel_s, ag_r, cross_r, tile_r, d2d_r, hop_r, end_r):
    chips = ep_size // CORES
    tok, dim = hid.shape
    n_exp, _, inter = wg.shape
    top_k = ids.shape[0]
    half = dim // 2
    rows = ep_size * tok
    n_blk = dim // COLS
    hc = COLS // 2
    pairs = n_exp * cap

    me = lax.axis_index("ep")
    chip, core = me // CORES, me % CORES
    other = 1 - core
    right, left, opp = (chip + 1) % chips, (chip + chips - 1) % chips, (chip + 2) % chips

    def slot(a_chip, a_core, at_chip=chip, at_core=core):
        away = (a_chip - at_chip + chips) % chips
        pos = away + away // 2 - 2 * (away // 3)
        cross_core = (a_core + at_core) % CORES
        is_far = pos // POS_FAR
        return pos + (chips - 1) * cross_core + is_far * (chips - 1 - (chips - 2) * cross_core)

    def dev(a_chip, a_core):
        return {"ep": a_chip * CORES + a_core}

    def remote(src, dst, to, s_sem, r_sem):
        copy = pltpu.make_async_remote_copy(src, dst, s_sem, r_sem, device_id=to, device_id_type=MESH)
        copy.start()
        return copy

    def await_all(ref, sem):
        pltpu.make_async_copy(ref, ref, sem).wait()

    ins = [pltpu.make_async_copy(s, d, in_sem.at[i]) for i, (s, d) in enumerate(((hid_h, hid), (gain_h, gain), (rw_h, rw), (ids_h, ids)))]
    for copy in ins:
        copy.start()
    early, late = slice(0, COLS), slice(COLS, dim)
    fetches = ((wg_h, wg), (wu_h, wu), (wd_h.at[:, :, early], wd.at[:, :, early]), (wd_h.at[:, :, late], wd.at[:, :, late]), (sg_h, sg), (su_h, su), (sd_h, sd))
    weights = []
    for i, (s, d) in enumerate(fetches):
        weights.append(pltpu.make_async_copy(s, d, w_sem.at[i]))
        weights[-1].start(priority=1)

    barrier = pltpu.get_barrier_semaphore()
    for k in range(1, ep_size):
        pl.semaphore_signal(barrier, inc=1, device_id={"ep": (me + k) % ep_size}, device_id_type=MESH)

    with jax.named_scope("norm"):
        ins[0].wait()
        ins[1].wait()
        x_f32 = hid[...].astype(F32)
        inv_rms = lax.rsqrt(jnp.mean(x_f32 * x_f32, axis=-1, keepdims=True) + NORM_EPS)
        gain_row = jnp.concatenate([gain[i : i + 1, :] for i in range(dim // 128)], axis=1)
        x_norm = (x_f32 * inv_rms * gain_row).astype(BF16)
        x_all[0] = x_norm

    with jax.named_scope("barwait"):
        pl.semaphore_wait(barrier, ep_size - 1)

    half = dim // 2
    q = [slice(k * half // 2, (k + 1) * half // 2) for k in range(4)]
    part_a, part_b = slice(0, half), slice(half, dim)

    def spread(a_chip, cols, to, r_sem):
        src, dst = x_all.at[slot(a_chip, core), :, cols], x_all.at[slot(a_chip, core, to, core), :, cols]
        return remote(src, dst, dev(to, core), ring_s, r_sem)

    def cross(a_chip, cols, r_sem):
        src, dst = x_all.at[slot(a_chip, core), :, cols], x_all.at[slot(a_chip, core, chip, other), :, cols]
        remote(src, dst, dev(chip, other), cross_s, r_sem)

    ra, lb = [], []
    for k in range(2):
        ra.append(spread(chip, q[k], right, ag_r.at[k]))
        lb.append(spread(chip, q[2 + k], left, ag_r.at[2 + k]))

    with jax.named_scope("router"):
        ins[2].wait()
        ins[3].wait()
        r_hi, r_mid, r_low = split3(rw[...])
        logits = (dot_t(r_low, x_norm) + dot_t(r_mid, x_norm)) + dot_t(r_hi, x_norm)
        scores = 1.0 / (1.0 + jnp.exp(-logits))
        exp_no = lax.broadcasted_iota(jnp.int32, logits.shape, 0)
        chosen = exp_no == ids[0:1, :]
        for k in range(1, top_k):
            chosen = jnp.logical_or(chosen, exp_no == ids[k : k + 1, :])
        total = jnp.sum(jnp.where(chosen, scores, 0.0), axis=0, keepdims=True)
        gates = jnp.where(chosen, ROUTE_SCALE * scores / total, -1.0)
        gt_send[...] = jnp.full(gt_send.shape, -1.0, F32)
        for d in range(ep_size):
            gt_send[d, :, 0:tok] = gates[d * n_exp : (d + 1) * n_exp, :]
        gt_all[0] = gt_send[me]
        for k in range(1, ep_size):
            to = (me + k) % ep_size
            remote(gt_send.at[to], gt_all.at[slot(chip, core, to // CORES, to % CORES)], {"ep": to}, tile_s, tile_r)

    rb = spread(chip, part_b, right, ag_r.at[4])
    la = spread(chip, part_a, left, ag_r.at[5])
    cross(chip, slice(0, dim), cross_r.at[0])

    with jax.named_scope("relays"):
        for k in range(2):
            ra[k].wait_recv()
            spread(left, q[k], right, ag_r.at[6])
            cross(left, q[k], cross_r.at[1])
            lb[k].wait_recv()
            spread(right, q[2 + k], left, ag_r.at[7])
            cross(right, q[2 + k], cross_r.at[1])

    def near_rest():
        rb.wait_recv()
        cross(left, part_b, cross_r.at[1])
        la.wait_recv()
        cross(right, part_a, cross_r.at[1])

    with jax.named_scope("tilewait"):
        await_all(gt_all.at[0 : ep_size - 1], tile_r)

    with jax.named_scope("onehot"):
        lane_src = lax.broadcasted_iota(jnp.int32, (n_exp, rows), 1) // tok
        gmat = jnp.full((n_exp, rows), -1.0, F32)
        for s in range(ep_size):
            wide = jnp.concatenate([gt_all[s], jnp.full((n_exp, rows - gt_all.shape[2]), -1.0, F32)], axis=1)
            if s:
                wide = pltpu.roll(wide, s * tok, 1)
            gmat = jnp.where(lane_src == s, wide, gmat)
        picked = jnp.logical_not(gmat < 0.0)
        upper = lax.broadcasted_iota(jnp.int32, (rows, rows), 0) < lax.broadcasted_iota(jnp.int32, (rows, rows), 1)
        rank = dot(jnp.where(picked, 1.0, 0.0).astype(BF16), jnp.where(upper, 1.0, 0.0).astype(BF16))
        place = jnp.where(picked, rank, -1.0)
        for i in range(pairs // 128):
            e_one, e_two = i * 128 // cap, (i * 128 + 127) // cap
            row_no = lax.broadcasted_iota(jnp.int32, (128, rows), 0) + i * 128
            first = row_no < e_two * cap
            pos = (row_no - jnp.where(first, e_one * cap, e_two * cap)).astype(F32)
            hit = pos == jnp.where(first, place[e_one : e_one + 1, :], place[e_two : e_two + 1, :])
            gated = jnp.where(hit, jnp.where(first, gmat[e_one : e_one + 1, :], gmat[e_two : e_two + 1, :]), 0.0)
            p_all[i * 128 : (i + 1) * 128, :] = jnp.where(hit, 1.0, 0.0).astype(BF16)
            for k, term in enumerate(reversed(split3(gated.T))):
                for b in range(ep_size):
                    to_row = S_ROW[b] * tok
                    acat[to_row : to_row + tok, k * pairs + i * 128 : k * pairs + (i + 1) * 128] = term[b * tok : (b + 1) * tok, :]

    n_near = rows // 2
    with jax.named_scope("nearrest"):
        near_rest()
    with jax.named_scope("nearwait"):
        await_all(x_all.at[0], cross_r.at[0])
    with jax.named_scope("near"):
        xg[...] = dot(p_all[:, 0:n_near], x_all[0 : ep_size // 2].reshape(n_near, dim)).astype(BF16)
    with jax.named_scope("far"):
        await_all(x_all.at[0, :, part_a], ag_r.at[6])
        cross(opp, part_a, cross_r.at[1])
        await_all(x_all.at[0, :, part_b], ag_r.at[7])
        cross(opp, part_b, cross_r.at[1])
    with jax.named_scope("farwait"):
        await_all(x_all.at[0 : chips - 1], cross_r.at[1])
        for copy in weights[:3]:
            copy.wait()

    part = []

    def last(j):
        cols = slice(j * COLS, (j + 1) * COLS)
        for e in range(n_exp):
            y = dot(hbuf[e * cap : (e + 1) * cap, :], wd[e, :, cols]).astype(BF16)
            for k in range(3):
                ybuf[j % 2, k * pairs + e * cap : k * pairs + (e + 1) * cap, :] = y

    def compute(j):
        if j == 1:
            last(1)
        if j and j + 1 < n_blk:
            last(j + 1)
        for k in range(CORES):
            sbuf[j, k] = dot(acat[k * chips * tok : (k + 1) * chips * tok, :], ybuf[j % 2])
        part.append(remote(sbuf.at[j, 1], d2d.at[j], dev(chip, other), d2d_s, d2d_r.at[j]))

    lo, up = slice(0, hc), slice(hc, COLS)
    half_blk = n_blk // 2

    def send(j):
        part[j].wait_recv()
        tbuf[j] = (sbuf[j, 0] + d2d[j]).reshape(chips, tok, COLS)
        remote(tbuf.at[j, POS_FAR, :, lo], hop.at[j, :, lo], dev(right, core), hop_s, hop_r.at[j])
        remote(tbuf.at[j, POS_FAR, :, up], hop.at[j, :, up], dev(left, core), hop_s, hop_r.at[j])

    def direct(j):
        remote(tbuf.at[j, POS_RIGHT, :, up], froml.at[j, :, up], dev(right, core), dir_s, end_r.at[0, j // half_blk])
        remote(tbuf.at[j, POS_LEFT, :, lo], fromr.at[j, :, lo], dev(left, core), dir_s, end_r.at[1, j // half_blk])

    def relay(j):
        await_all(hop.at[j], hop_r.at[j])
        rel[j, :, lo] = hop[j, :, lo] + tbuf[j, POS_RIGHT, :, lo]
        rel[j, :, up] = hop[j, :, up] + tbuf[j, POS_LEFT, :, up]
        remote(rel.at[j, :, lo], froml.at[j, :, lo], dev(right, core), rel_s, end_r.at[0, j // half_blk])
        remote(rel.at[j, :, up], fromr.at[j, :, up], dev(left, core), rel_s, end_r.at[1, j // half_blk])

    def finish(k):
        blks = slice(k * half_blk, (k + 1) * half_blk)
        await_all(froml.at[blks], end_r.at[0, k])
        await_all(fromr.at[blks], end_r.at[1, k])
        for j in range(k * half_blk, (k + 1) * half_blk):
            cols = slice(j * COLS, (j + 1) * COLS)
            routed = (tbuf[j, POS_OWN] + froml[j]) + fromr[j]
            out_ref[:, cols] = ((hid[:, cols].astype(F32) + shared[:, cols].astype(F32)) + routed).astype(BF16)

    def scoped(f, j):
        with jax.named_scope(f"{f.__name__}{j}"):
            f(j)

    with jax.named_scope("gateup"):
        x_far = x_all[ep_size // 2 : ep_size].reshape(rows - n_near, dim)
        for e in range(n_exp):
            if e % 2 == 0:
                two = slice(e * cap, (e + 2) * cap)
                xg[two, :] = xg[two, :] + dot(p_all[two, n_near:], x_far).astype(BF16)
            own = slice(e * cap, (e + 1) * cap)
            h_gate = dot(xg[own, :], wg[e])
            h_up = dot(xg[own, :], wu[e])
            hbuf[own, :] = (jax.nn.silu(h_gate) * h_up).astype(BF16)
        last(0)
        compute(0)
    weights[3].wait()
    for j in range(n_blk):
        if j:
            scoped(compute, j)
        if j >= 1:
            scoped(send, j - 1)
            scoped(direct, j - 1)
    scoped(send, n_blk - 1)

    with jax.named_scope("shared"):
        for copy in weights[4:]:
            copy.wait()
        xs = x_all[0]
        mid_cols = hsh.shape[1] // 2

        def shared_part(k):
            cols = slice(k * mid_cols, (k + 1) * mid_cols)
            hsh[:, cols] = (jax.nn.silu(dot(xs, sg[:, cols])) * dot(xs, su[:, cols])).astype(BF16)

        scoped(relay, 0)
        scoped(relay, 1)
        scoped(direct, n_blk - 1)
        shared_part(0)
        scoped(relay, 2)
        scoped(relay, 3)
        shared_part(1)
        scoped(relay, 4)
        scoped(relay, 5)
        shared[...] = dot(hsh[...], sd[...]).astype(BF16)
    for k in range(2):
        scoped(finish, k)
    with jax.named_scope("drain"):
        await_all(x_all.at[0:3], ring_s)
        await_all(x_all.at[0:chips], cross_s)
        await_all(gt_send.at[0 : ep_size - 1], tile_s)
        await_all(d2d, d2d_s)
        await_all(hop, hop_s)
        await_all(froml, dir_s)
        await_all(rel, rel_s)


def put_kernel(src, dst, o_sem):
    copy = pltpu.make_async_copy(src, dst, o_sem)
    copy.start()
    copy.wait()


def solution(mesh):
    ep_size = mesh.shape["ep"]

    def local_block(hidden_in, norm_gain, router_w, w_gate, w_up, w_down, ws_gate, ws_up, ws_down, expert_ids):
        tok, top_k = expert_ids.shape
        dim = hidden_in.shape[1]
        n_exp, _, inter = w_gate.shape
        s_inter = ws_gate.shape[1]
        cap = GROUPS * ((top_k + GROUP_LIMIT - 1) // GROUP_LIMIT) * tok // n_exp
        rows = ep_size * tok
        pairs = n_exp * cap
        n_blk = dim // COLS
        chips = ep_size // CORES
        vm, sem = pltpu.VMEM, pltpu.SemaphoreType.DMA
        scratch = [
            vm((tok, dim), BF16), vm((dim // 128, 128), F32), vm(router_w.shape, F32), vm((top_k, tok), jnp.int32),
            vm(w_gate.shape, BF16), vm(w_up.shape, BF16), vm(w_down.shape, BF16),
            vm(ws_gate.shape, BF16), vm(ws_up.shape, BF16), vm(ws_down.shape, BF16),
            vm((ep_size, tok, dim), BF16), vm((ep_size, n_exp, 128), F32), vm((ep_size, n_exp, 128), F32),
            vm((pairs, rows), BF16),
            vm((rows, 3 * pairs), BF16),
            vm((pairs, dim), BF16), vm((pairs, inter), BF16), vm((2, 3 * pairs, COLS), BF16),
            vm((n_blk, CORES, chips * tok, COLS), F32), vm((n_blk, chips * tok, COLS), F32), vm((n_blk, chips, tok, COLS), F32),
            vm((n_blk, tok, COLS), F32), vm((n_blk, tok, COLS), F32), vm((n_blk, tok, COLS), F32), vm((n_blk, tok, COLS), F32),
            vm((tok, s_inter), BF16), vm((tok, dim), BF16),
            sem((4,)), sem((7,)), sem, sem, sem, sem, sem, sem, sem,
            sem((8,)), sem((2,)), sem, sem((n_blk,)), sem((n_blk,)), sem((2, 2)),
        ]
        result = pl.pallas_call(
            functools.partial(moe_kernel, ep_size, cap),
            out_shape=pltpu.VMEM((tok, dim), BF16),
            in_specs=[pl.BlockSpec(memory_space=pl.ANY)] * 10,
            out_specs=pl.BlockSpec(memory_space=pltpu.VMEM),
            scratch_shapes=scratch,
            compiler_params=pltpu.CompilerParams(collective_id=0, has_side_effects=True, vmem_limit_bytes=64_900_000),
            name="moe_block",
        )(hidden_in, norm_gain.reshape(dim // 128, 128), router_w, w_gate, w_up, w_down, ws_gate, ws_up, ws_down, expert_ids.T)
        return result

    row_spec = P(("dp", "ep"), None)
    in_specs = (row_spec, P(), P(), P("ep"), P("ep"), P("ep"), P(), P(), P(), row_spec)
    return jax.shard_map(local_block, mesh=mesh, in_specs=in_specs, out_specs=row_spec, check_vma=False)
```

```python
import functools

import jax
import jax.numpy as jnp
from jax import lax
from jax.experimental import pallas as pl
from jax.experimental.pallas import tpu as pltpu
from jax.sharding import PartitionSpec as P

NORM_EPS = 1e-6
ROUTE_SCALE = 2.5
GROUPS = 8
GROUP_LIMIT = 4
CORES = 2
S_ROW = (0, 1, 2, 4, 5, 6, 3, 7)
POS_OWN, POS_RIGHT, POS_LEFT, POS_FAR = range(4)
COLS = 256
CHUNK = 512
MESH = pl.DeviceIdType.MESH
F32 = jnp.float32
BF16 = jnp.bfloat16


def dot(a, b):
    return jnp.dot(a, b, preferred_element_type=F32)


def dot_t(a, b):
    return lax.dot_general(a, b, (((1,), (1,)), ((), ())), preferred_element_type=F32)


def split3(v):
    hi = v.astype(BF16)
    rest = v - hi.astype(F32)
    mid = rest.astype(BF16)
    low = (rest - mid.astype(F32)).astype(BF16)
    return hi, mid, low


def moe_kernel(ep_size, cap, hid_h, gain_h, rw_h, wg_h, wu_h, wd_h, sg_h, su_h, sd_h, ids_h, out_ref,
               hid, gain, rw, ids, wg, wu, wd, sg, su, sd, x_all, gt_send, gt_all, p_all, acat,
               xg, hbuf, ybuf, sbuf, d2d, tbuf, hop, rel, froml, fromr, hsh, shared,
               in_sem, w_sem,
               ring_s, cross_s, tile_s, d2d_s, hop_s, dir_s, rel_s, ag_r, cross_r, tile_r, d2d_r, hop_r, end_r):
    chips = ep_size // CORES
    tok, dim = hid.shape
    n_exp, _, inter = wg.shape
    top_k = ids.shape[0]
    half = dim // 2
    rows = ep_size * tok
    n_blk = dim // COLS
    hc = COLS // 2
    pairs = n_exp * cap

    me = lax.axis_index("ep")
    chip, core = me // CORES, me % CORES
    other = 1 - core
    right, left, opp = (chip + 1) % chips, (chip + chips - 1) % chips, (chip + 2) % chips

    def slot(a_chip, a_core, at_chip=chip, at_core=core):
        away = (a_chip - at_chip + chips) % chips
        pos = away + away // 2 - 2 * (away // 3)
        cross_core = (a_core + at_core) % CORES
        is_far = pos // POS_FAR
        return pos + (chips - 1) * cross_core + is_far * (chips - 1 - (chips - 2) * cross_core)

    def dev(a_chip, a_core):
        return {"ep": a_chip * CORES + a_core}

    def remote(src, dst, to, s_sem, r_sem):
        copy = pltpu.make_async_remote_copy(src, dst, s_sem, r_sem, device_id=to, device_id_type=MESH)
        copy.start()
        return copy

    def await_all(ref, sem):
        pltpu.make_async_copy(ref, ref, sem).wait()

    ins = [pltpu.make_async_copy(s, d, in_sem.at[i]) for i, (s, d) in enumerate(((hid_h, hid), (gain_h, gain), (rw_h, rw), (ids_h, ids)))]
    for copy in ins:
        copy.start()
    early, late = slice(0, COLS), slice(COLS, dim)
    chunk = (slice(0, CHUNK), slice(CHUNK, dim))
    fetches = [(h.at[:, rng, :], v.at[:, rng, :]) for rng in chunk for h, v in ((wg_h, wg), (wu_h, wu))]
    fetches += [(wd_h.at[:, :, early], wd.at[:, :, early]), (wd_h.at[:, :, late], wd.at[:, :, late]), (sg_h, sg), (su_h, su), (sd_h, sd)]
    weights = []
    for i, (s, d) in enumerate(fetches):
        weights.append(pltpu.make_async_copy(s, d, w_sem.at[i]))
        weights[-1].start(priority=1)

    barrier = pltpu.get_barrier_semaphore()
    for k in range(1, ep_size):
        pl.semaphore_signal(barrier, inc=1, device_id={"ep": (me + k) % ep_size}, device_id_type=MESH)

    with jax.named_scope("norm"):
        ins[0].wait()
        ins[1].wait()
        x_f32 = hid[...].astype(F32)
        inv_rms = lax.rsqrt(jnp.mean(x_f32 * x_f32, axis=-1, keepdims=True) + NORM_EPS)
        gain_row = jnp.concatenate([gain[i : i + 1, :] for i in range(dim // 128)], axis=1)
        x_norm = (x_f32 * inv_rms * gain_row).astype(BF16)
        x_all[0] = x_norm

    with jax.named_scope("barwait"):
        pl.semaphore_wait(barrier, ep_size - 1)

    side_a = [slice(0, CHUNK // 2), slice(CHUNK, (CHUNK + dim) // 2)]
    side_b = [slice(CHUNK // 2, CHUNK), slice((CHUNK + dim) // 2, dim)]

    def spread(a_chip, cols, to, r_sem):
        src, dst = x_all.at[slot(a_chip, core), :, cols], x_all.at[slot(a_chip, core, to, core), :, cols]
        return remote(src, dst, dev(to, core), ring_s, r_sem)

    def cross(a_chip, cols, r_sem):
        src, dst = x_all.at[slot(a_chip, core), :, cols], x_all.at[slot(a_chip, core, chip, other), :, cols]
        remote(src, dst, dev(chip, other), cross_s, r_sem)

    ra, lb = [], []
    for k in range(2):
        ra.append(spread(chip, side_a[k], right, ag_r.at[k]))
        lb.append(spread(chip, side_b[k], left, ag_r.at[2 + k]))

    with jax.named_scope("router"):
        ins[2].wait()
        ins[3].wait()
        r_hi, r_mid, r_low = split3(rw[...])
        logits = (dot_t(r_low, x_norm) + dot_t(r_mid, x_norm)) + dot_t(r_hi, x_norm)
        scores = 1.0 / (1.0 + jnp.exp(-logits))
        exp_no = lax.broadcasted_iota(jnp.int32, logits.shape, 0)
        chosen = exp_no == ids[0:1, :]
        for k in range(1, top_k):
            chosen = jnp.logical_or(chosen, exp_no == ids[k : k + 1, :])
        total = jnp.sum(jnp.where(chosen, scores, 0.0), axis=0, keepdims=True)
        gates = jnp.where(chosen, ROUTE_SCALE * scores / total, -1.0)
        gt_send[...] = jnp.full(gt_send.shape, -1.0, F32)
        for d in range(ep_size):
            gt_send[d, :, 0:tok] = gates[d * n_exp : (d + 1) * n_exp, :]
        gt_all[0] = gt_send[me]
        for k in range(1, ep_size):
            to = (me + k) % ep_size
            remote(gt_send.at[to], gt_all.at[slot(chip, core, to // CORES, to % CORES)], {"ep": to}, tile_s, tile_r)

    for k in range(2):
        spread(chip, side_b[k], right, ag_r.at[4])
        spread(chip, side_a[k], left, ag_r.at[5])
    cross(chip, slice(0, dim), cross_r.at[0])

    with jax.named_scope("relays"):
        for k in range(2):
            ra[k].wait_recv()
            spread(left, side_a[k], right, ag_r.at[6 + 2 * k])
            cross(left, side_a[k], cross_r.at[1])
            lb[k].wait_recv()
            spread(right, side_b[k], left, ag_r.at[7 + 2 * k])
            cross(right, side_b[k], cross_r.at[1])

    def near_rest():
        await_all(x_all.at[0, :, 0 : dim // 2], ag_r.at[4])
        await_all(x_all.at[0, :, 0 : dim // 2], ag_r.at[5])
        for k in range(2):
            cross(left, side_b[k], cross_r.at[1])
            cross(right, side_a[k], cross_r.at[1])

    with jax.named_scope("tilewait"):
        await_all(gt_all.at[0 : ep_size - 1], tile_r)

    with jax.named_scope("onehot"):
        lane_src = lax.broadcasted_iota(jnp.int32, (n_exp, rows), 1) // tok
        gmat = jnp.full((n_exp, rows), -1.0, F32)
        for s in range(ep_size):
            wide = jnp.concatenate([gt_all[s], jnp.full((n_exp, rows - gt_all.shape[2]), -1.0, F32)], axis=1)
            if s:
                wide = pltpu.roll(wide, s * tok, 1)
            gmat = jnp.where(lane_src == s, wide, gmat)
        picked = jnp.logical_not(gmat < 0.0)
        upper = lax.broadcasted_iota(jnp.int32, (rows, rows), 0) < lax.broadcasted_iota(jnp.int32, (rows, rows), 1)
        rank = dot(jnp.where(picked, 1.0, 0.0).astype(BF16), jnp.where(upper, 1.0, 0.0).astype(BF16))
        place = jnp.where(picked, rank, -1.0)
        for i in range(pairs // 128):
            e_one, e_two = i * 128 // cap, (i * 128 + 127) // cap
            row_no = lax.broadcasted_iota(jnp.int32, (128, rows), 0) + i * 128
            first = row_no < e_two * cap
            pos = (row_no - jnp.where(first, e_one * cap, e_two * cap)).astype(F32)
            hit = pos == jnp.where(first, place[e_one : e_one + 1, :], place[e_two : e_two + 1, :])
            gated = jnp.where(hit, jnp.where(first, gmat[e_one : e_one + 1, :], gmat[e_two : e_two + 1, :]), 0.0)
            p_all[i * 128 : (i + 1) * 128, :] = jnp.where(hit, 1.0, 0.0).astype(BF16)
            for k, term in enumerate(reversed(split3(gated.T))):
                for b in range(ep_size):
                    to_row = S_ROW[b] * tok
                    acat[to_row : to_row + tok, k * pairs + i * 128 : k * pairs + (i + 1) * 128] = term[b * tok : (b + 1) * tok, :]

    n_near = rows // 2
    with jax.named_scope("nearrest"):
        near_rest()
    with jax.named_scope("nearwait"):
        await_all(x_all.at[0], cross_r.at[0])
    x_near = x_all.at[0 : ep_size // 2]
    x_rest = x_all.at[ep_size // 2 : ep_size]

    def gather_near(k):
        with jax.named_scope(f"near{k}"):
            xg[:, chunk[k]] = dot(p_all[:, 0:n_near], x_near[:, :, chunk[k]].reshape(n_near, -1)).astype(BF16)

    def pass_far(k):
        with jax.named_scope(f"far{k}"):
            await_all(x_all.at[0, :, side_a[k]], ag_r.at[6 + 2 * k])
            await_all(x_all.at[0, :, side_b[k]], ag_r.at[7 + 2 * k])
            cross(opp, chunk[k], cross_r.at[2 + k])

    def gate_up(k):
        def gather_far(p):
            two = slice(2 * p * cap, 2 * (p + 1) * cap)
            xg[two, chunk[k]] = xg[two, chunk[k]] + dot(p_all[two, n_near:], x_rest[:, :, chunk[k]].reshape(rows - n_near, -1)).astype(BF16)

        gather_far(0)
        for e in range(n_exp):
            if e % 2 == 0 and e + 2 < n_exp:
                gather_far(e // 2 + 1)
            own = slice(e * cap, (e + 1) * cap)
            row = e % 4 * cap
            xe = xg[own, chunk[k]]
            h = []
            for m, w in enumerate((wg, wu)):
                total_h = dot(xe, w[e, chunk[k], :])
                for c in range(2):
                    spot = sbuf.at[4 * m + 2 * c + e // 4, row // (chips * tok), row % (chips * tok) : row % (chips * tok) + cap, :]
                    piece = total_h[:, c * COLS : (c + 1) * COLS]
                    if k == 0:
                        spot[...] = piece
                    else:
                        h.append(spot[...] + piece)
            if k:
                for c in range(2):
                    hbuf[own, c * COLS : (c + 1) * COLS] = (jax.nn.silu(h[c]) * h[2 + c]).astype(BF16)

    gather_near(0)
    pass_far(0)
    gather_near(1)
    pass_far(1)
    with jax.named_scope("farwait0"):
        await_all(x_all.at[0 : chips - 2], cross_r.at[1])
        await_all(x_all.at[0, :, chunk[0]], cross_r.at[2])
        weights[0].wait()
        weights[1].wait()
    with jax.named_scope("gateup0"):
        gate_up(0)
    with jax.named_scope("farwait1"):
        await_all(x_all.at[0, :, chunk[1]], cross_r.at[3])
        for copy in weights[2:5]:
            copy.wait()

    part = []

    def last(j):
        cols = slice(j * COLS, (j + 1) * COLS)
        for e in range(n_exp):
            y = dot(hbuf[e * cap : (e + 1) * cap, :], wd[e, :, cols]).astype(BF16)
            for k in range(3):
                ybuf[j % 2, k * pairs + e * cap : k * pairs + (e + 1) * cap, :] = y

    def compute(j):
        if j == 1:
            last(1)
        if j and j + 1 < n_blk:
            last(j + 1)
        for k in range(CORES):
            sbuf[j, k] = dot(acat[k * chips * tok : (k + 1) * chips * tok, :], ybuf[j % 2])
        part.append(remote(sbuf.at[j, 1], d2d.at[j], dev(chip, other), d2d_s, d2d_r.at[j]))

    lo, up = slice(0, hc), slice(hc, COLS)
    half_blk = n_blk // 2

    def send(j):
        part[j].wait_recv()
        tbuf[j] = (sbuf[j, 0] + d2d[j]).reshape(chips, tok, COLS)
        remote(tbuf.at[j, POS_FAR, :, lo], hop.at[j, :, lo], dev(right, core), hop_s, hop_r.at[j])
        remote(tbuf.at[j, POS_FAR, :, up], hop.at[j, :, up], dev(left, core), hop_s, hop_r.at[j])

    def direct(j):
        remote(tbuf.at[j, POS_RIGHT, :, up], froml.at[j, :, up], dev(right, core), dir_s, end_r.at[0, j // half_blk])
        remote(tbuf.at[j, POS_LEFT, :, lo], fromr.at[j, :, lo], dev(left, core), dir_s, end_r.at[1, j // half_blk])

    def relay(j):
        await_all(hop.at[j], hop_r.at[j])
        rel[j, :, lo] = hop[j, :, lo] + tbuf[j, POS_RIGHT, :, lo]
        rel[j, :, up] = hop[j, :, up] + tbuf[j, POS_LEFT, :, up]
        remote(rel.at[j, :, lo], froml.at[j, :, lo], dev(right, core), rel_s, end_r.at[0, j // half_blk])
        remote(rel.at[j, :, up], fromr.at[j, :, up], dev(left, core), rel_s, end_r.at[1, j // half_blk])

    def finish(k):
        blks = slice(k * half_blk, (k + 1) * half_blk)
        await_all(froml.at[blks], end_r.at[0, k])
        await_all(fromr.at[blks], end_r.at[1, k])
        for j in range(k * half_blk, (k + 1) * half_blk):
            cols = slice(j * COLS, (j + 1) * COLS)
            routed = (tbuf[j, POS_OWN] + froml[j]) + fromr[j]
            out_ref[:, cols] = ((hid[:, cols].astype(F32) + shared[:, cols].astype(F32)) + routed).astype(BF16)

    def scoped(f, j):
        with jax.named_scope(f"{f.__name__}{j}"):
            f(j)

    with jax.named_scope("gateup1"):
        gate_up(1)
        last(0)
        compute(0)
    weights[5].wait()
    for j in range(n_blk):
        if j:
            scoped(compute, j)
        if j >= 1:
            scoped(send, j - 1)
            scoped(direct, j - 1)
    scoped(send, n_blk - 1)

    with jax.named_scope("shared"):
        for copy in weights[6:]:
            copy.wait()
        xs = x_all[0]
        mid_cols = hsh.shape[1] // 2

        def shared_part(k):
            cols = slice(k * mid_cols, (k + 1) * mid_cols)
            hsh[:, cols] = (jax.nn.silu(dot(xs, sg[:, cols])) * dot(xs, su[:, cols])).astype(BF16)

        scoped(relay, 0)
        scoped(relay, 1)
        scoped(direct, n_blk - 1)
        shared_part(0)
        scoped(relay, 2)
        scoped(relay, 3)
        shared_part(1)
        scoped(relay, 4)
        scoped(relay, 5)
        shared[...] = dot(hsh[...], sd[...]).astype(BF16)
    for k in range(2):
        scoped(finish, k)
    with jax.named_scope("drain"):
        await_all(x_all.at[0:3], ring_s)
        await_all(x_all.at[0:chips], cross_s)
        await_all(gt_send.at[0 : ep_size - 1], tile_s)
        await_all(d2d, d2d_s)
        await_all(hop, hop_s)
        await_all(froml, dir_s)
        await_all(rel, rel_s)


def put_kernel(src, dst, o_sem):
    copy = pltpu.make_async_copy(src, dst, o_sem)
    copy.start()
    copy.wait()


def solution(mesh):
    ep_size = mesh.shape["ep"]

    def local_block(hidden_in, norm_gain, router_w, w_gate, w_up, w_down, ws_gate, ws_up, ws_down, expert_ids):
        tok, top_k = expert_ids.shape
        dim = hidden_in.shape[1]
        n_exp, _, inter = w_gate.shape
        s_inter = ws_gate.shape[1]
        cap = GROUPS * ((top_k + GROUP_LIMIT - 1) // GROUP_LIMIT) * tok // n_exp
        rows = ep_size * tok
        pairs = n_exp * cap
        n_blk = dim // COLS
        chips = ep_size // CORES
        vm, sem = pltpu.VMEM, pltpu.SemaphoreType.DMA
        scratch = [
            vm((tok, dim), BF16), vm((dim // 128, 128), F32), vm(router_w.shape, F32), vm((top_k, tok), jnp.int32),
            vm(w_gate.shape, BF16), vm(w_up.shape, BF16), vm(w_down.shape, BF16),
            vm(ws_gate.shape, BF16), vm(ws_up.shape, BF16), vm(ws_down.shape, BF16),
            vm((ep_size, tok, dim), BF16), vm((ep_size, n_exp, 128), F32), vm((ep_size, n_exp, 128), F32),
            vm((pairs, rows), BF16),
            vm((rows, 3 * pairs), BF16),
            vm((pairs, dim), BF16), vm((pairs, inter), BF16), vm((2, 3 * pairs, COLS), BF16),
            vm((8, CORES, chips * tok, COLS), F32), vm((n_blk, chips * tok, COLS), F32), vm((n_blk, chips, tok, COLS), F32),
            vm((n_blk, tok, COLS), F32), vm((n_blk, tok, COLS), F32), vm((n_blk, tok, COLS), F32), vm((n_blk, tok, COLS), F32),
            vm((tok, s_inter), BF16), vm((tok, dim), BF16),
            sem((4,)), sem((9,)), sem, sem, sem, sem, sem, sem, sem,
            sem((10,)), sem((4,)), sem, sem((n_blk,)), sem((n_blk,)), sem((2, 2)),
        ]
        result = pl.pallas_call(
            functools.partial(moe_kernel, ep_size, cap),
            out_shape=pltpu.VMEM((tok, dim), BF16),
            in_specs=[pl.BlockSpec(memory_space=pl.ANY)] * 10,
            out_specs=pl.BlockSpec(memory_space=pltpu.VMEM),
            scratch_shapes=scratch,
            compiler_params=pltpu.CompilerParams(collective_id=0, has_side_effects=True, vmem_limit_bytes=65_800_000),
            name="moe_block",
        )(hidden_in, norm_gain.reshape(dim // 128, 128), router_w, w_gate, w_up, w_down, ws_gate, ws_up, ws_down, expert_ids.T)
        return result

    row_spec = P(("dp", "ep"), None)
    in_specs = (row_spec, P(), P(), P("ep"), P("ep"), P("ep"), P(), P(), P(), row_spec)
    return jax.shard_map(local_block, mesh=mesh, in_specs=in_specs, out_specs=row_spec, check_vma=False)
```

```python
import functools

import jax
import jax.numpy as jnp
from jax import lax
from jax.experimental import pallas as pl
from jax.experimental.pallas import tpu as pltpu
from jax.sharding import PartitionSpec as P

NORM_EPS = 1e-6
ROUTE_SCALE = 2.5
GROUPS = 8
GROUP_LIMIT = 4
CORES = 2
HUB = 1
S_ROW = (0, 1, 2, 4, 5, 6, 3, 7)
POS_OWN, POS_RIGHT, POS_LEFT, POS_FAR = range(4)
COLS = 256
CHUNK = 512
MESH = pl.DeviceIdType.MESH
F32 = jnp.float32
BF16 = jnp.bfloat16


def dot(a, b):
    return jnp.dot(a, b, preferred_element_type=F32)


def dot_t(a, b):
    return lax.dot_general(a, b, (((1,), (1,)), ((), ())), preferred_element_type=F32)


def split3(v):
    hi = v.astype(BF16)
    rest = v - hi.astype(F32)
    mid = rest.astype(BF16)
    low = (rest - mid.astype(F32)).astype(BF16)
    return hi, mid, low


def moe_kernel(ep_size, cap, hid_h, gain_h, rw_h, wg_h, wu_h, wd_h, sg_h, su_h, sd_h, ids_h, out_ref,
               hid, gain, rw, ids, wg, wu, wd, sg, su, sd, x_all, gt_send, gt_all, p_all, acat,
               xg, hbuf, ybuf, sbuf, d2d, tbuf, hop, rel, froml, fromr, hsh, shared,
               in_sem, w_sem,
               ring_s, cross_s, tile_s, d2d_s, hop_s, dir_s, rel_s, ag_r, cross_r, tile_r, d2d_r, hop_r, end_r):
    chips = ep_size // CORES
    tok, dim = hid.shape
    n_exp, _, inter = wg.shape
    top_k = ids.shape[0]
    half = dim // 2
    rows = ep_size * tok
    n_blk = dim // COLS
    hc = COLS // 2
    pairs = n_exp * cap

    me = lax.axis_index("ep")
    chip, core = me // CORES, me % CORES
    other = 1 - core
    right, left, opp = (chip + 1) % chips, (chip + chips - 1) % chips, (chip + 2) % chips

    def slot(a_chip, a_core, at_chip=chip, at_core=core):
        away = (a_chip - at_chip + chips) % chips
        pos = away + away // 2 - 2 * (away // 3)
        cross_core = (a_core + at_core) % CORES
        is_far = pos // POS_FAR
        return pos + (chips - 1) * cross_core + is_far * (chips - 1 - (chips - 2) * cross_core)

    def dev(a_chip, a_core):
        return {"ep": a_chip * CORES + a_core}

    def remote(src, dst, to, s_sem, r_sem):
        copy = pltpu.make_async_remote_copy(src, dst, s_sem, r_sem, device_id=to, device_id_type=MESH)
        copy.start()
        return copy

    def await_all(ref, sem):
        pltpu.make_async_copy(ref, ref, sem).wait()

    ins = [pltpu.make_async_copy(s, d, in_sem.at[i]) for i, (s, d) in enumerate(((hid_h, hid), (gain_h, gain), (rw_h, rw), (ids_h, ids)))]
    for copy in ins:
        copy.start()
    early, late = slice(0, COLS), slice(COLS, dim)
    chunk = (slice(0, CHUNK), slice(CHUNK, dim))
    fetches = [(h.at[:, rng, :], v.at[:, rng, :]) for rng in chunk for h, v in ((wg_h, wg), (wu_h, wu))]
    fetches += [(wd_h.at[:, :, early], wd.at[:, :, early]), (wd_h.at[:, :, late], wd.at[:, :, late]), (sg_h, sg), (su_h, su), (sd_h, sd)]
    weights = []
    for i, (s, d) in enumerate(fetches):
        weights.append(pltpu.make_async_copy(s, d, w_sem.at[i]))
        weights[-1].start(priority=1)

    barrier = pltpu.get_barrier_semaphore()
    for k in range(1, ep_size):
        pl.semaphore_signal(barrier, inc=1, device_id={"ep": (me + k) % ep_size}, device_id_type=MESH)

    with jax.named_scope("norm"):
        ins[0].wait()
        ins[1].wait()
        x_f32 = hid[...].astype(F32)
        inv_rms = lax.rsqrt(jnp.mean(x_f32 * x_f32, axis=-1, keepdims=True) + NORM_EPS)
        gain_row = jnp.concatenate([gain[i : i + 1, :] for i in range(dim // 128)], axis=1)
        x_norm = (x_f32 * inv_rms * gain_row).astype(BF16)
        x_all[0] = x_norm

    with jax.named_scope("barwait"):
        pl.semaphore_wait(barrier, ep_size - 1)

    side_a = [slice(0, CHUNK // 2), slice(CHUNK, (CHUNK + dim) // 2)]
    side_b = [slice(CHUNK // 2, CHUNK), slice((CHUNK + dim) // 2, dim)]

    def spread(a_chip, cols, to, r_sem, to_core=core):
        src, dst = x_all.at[slot(a_chip, core), :, cols], x_all.at[slot(a_chip, core, to, to_core), :, cols]
        return remote(src, dst, dev(to, to_core), ring_s, r_sem)

    def cross(a_chip, cols, r_sem):
        src, dst = x_all.at[slot(a_chip, core), :, cols], x_all.at[slot(a_chip, core, chip, other), :, cols]
        remote(src, dst, dev(chip, other), cross_s, r_sem)

    ra, lb = [], []
    for k in range(2):
        ra.append(spread(chip, side_a[k], right, ag_r.at[k]))
        lb.append(spread(chip, side_b[k], left, ag_r.at[2 + k]))

    with jax.named_scope("router"):
        ins[2].wait()
        ins[3].wait()
        r_hi, r_mid, r_low = split3(rw[...])
        logits = (dot_t(r_low, x_norm) + dot_t(r_mid, x_norm)) + dot_t(r_hi, x_norm)
        scores = 1.0 / (1.0 + jnp.exp(-logits))
        exp_no = lax.broadcasted_iota(jnp.int32, logits.shape, 0)
        chosen = exp_no == ids[0:1, :]
        for k in range(1, top_k):
            chosen = jnp.logical_or(chosen, exp_no == ids[k : k + 1, :])
        total = jnp.sum(jnp.where(chosen, scores, 0.0), axis=0, keepdims=True)
        gates = jnp.where(chosen, ROUTE_SCALE * scores / total, -1.0)
        gt_send[...] = jnp.full(gt_send.shape, -1.0, F32)
        for d in range(ep_size):
            gt_send[d, :, 0:tok] = gates[d * n_exp : (d + 1) * n_exp, :]
        gt_all[0] = gt_send[me]
        for k in range(1, ep_size):
            to = (me + k) % ep_size
            remote(gt_send.at[to], gt_all.at[slot(chip, core, to // CORES, to % CORES)], {"ep": to}, tile_s, tile_r)

    for k in range(2):
        spread(chip, side_b[k], right, ag_r.at[4])
        spread(chip, side_a[k], left, ag_r.at[5])
    cross(chip, slice(0, dim), cross_r.at[0])

    with jax.named_scope("relays"):
        for k in range(2):
            ra[k].wait_recv()
            spread(left, side_a[k], right, ag_r.at[6 + 2 * k], HUB)
            cross(left, side_a[k], cross_r.at[1])
            lb[k].wait_recv()
            spread(right, side_b[k], left, ag_r.at[7 + 2 * k], HUB)
            cross(right, side_b[k], cross_r.at[1])

    def near_rest():
        await_all(x_all.at[0, :, 0 : dim // 2], ag_r.at[4])
        await_all(x_all.at[0, :, 0 : dim // 2], ag_r.at[5])
        for k in range(2):
            cross(left, side_b[k], cross_r.at[1])
            cross(right, side_a[k], cross_r.at[1])

    with jax.named_scope("tilewait"):
        await_all(gt_all.at[0 : ep_size - 1], tile_r)

    with jax.named_scope("onehot"):
        lane_src = lax.broadcasted_iota(jnp.int32, (n_exp, rows), 1) // tok
        gmat = jnp.full((n_exp, rows), -1.0, F32)
        for s in range(ep_size):
            wide = jnp.concatenate([gt_all[s], jnp.full((n_exp, rows - gt_all.shape[2]), -1.0, F32)], axis=1)
            if s:
                wide = pltpu.roll(wide, s * tok, 1)
            gmat = jnp.where(lane_src == s, wide, gmat)
        picked = jnp.logical_not(gmat < 0.0)
        upper = lax.broadcasted_iota(jnp.int32, (rows, rows), 0) < lax.broadcasted_iota(jnp.int32, (rows, rows), 1)
        rank = dot(jnp.where(picked, 1.0, 0.0).astype(BF16), jnp.where(upper, 1.0, 0.0).astype(BF16))
        place = jnp.where(picked, rank, -1.0)
        for i in range(pairs // 128):
            e_one, e_two = i * 128 // cap, (i * 128 + 127) // cap
            row_no = lax.broadcasted_iota(jnp.int32, (128, rows), 0) + i * 128
            first = row_no < e_two * cap
            pos = (row_no - jnp.where(first, e_one * cap, e_two * cap)).astype(F32)
            hit = pos == jnp.where(first, place[e_one : e_one + 1, :], place[e_two : e_two + 1, :])
            gated = jnp.where(hit, jnp.where(first, gmat[e_one : e_one + 1, :], gmat[e_two : e_two + 1, :]), 0.0)
            p_all[i * 128 : (i + 1) * 128, :] = jnp.where(hit, 1.0, 0.0).astype(BF16)
            for k, term in enumerate(reversed(split3(gated.T))):
                for b in range(ep_size):
                    to_row = S_ROW[b] * tok
                    acat[to_row : to_row + tok, k * pairs + i * 128 : k * pairs + (i + 1) * 128] = term[b * tok : (b + 1) * tok, :]

    n_near = rows // 2
    with jax.named_scope("nearrest"):
        near_rest()
    with jax.named_scope("nearwait"):
        await_all(x_all.at[0], cross_r.at[0])
    x_near = x_all.at[0 : ep_size // 2]
    x_rest = x_all.at[ep_size // 2 : ep_size]

    far_slots = slice(ep_size - CORES, ep_size)

    def far_wait(k):
        @pl.when(core != HUB)
        def _():
            await_all(x_all.at[far_slots, :, chunk[k]], cross_r.at[2 + k])

    def gather_near(k):
        with jax.named_scope(f"near{k}"):
            xg[:, chunk[k]] = dot(p_all[:, 0:n_near], x_near[:, :, chunk[k]].reshape(n_near, -1)).astype(BF16)

    def pass_far(k):
        with jax.named_scope(f"far{k}"):
            @pl.when(core == HUB)
            def _():
                for r_sem, cols in ((6 + 2 * k, side_a[k]), (7 + 2 * k, side_b[k])):
                    await_all(x_all.at[far_slots, :, cols], ag_r.at[r_sem])
                for i in range(CORES):
                    src, dst = x_all.at[ep_size - 1 - i, :, chunk[k]], x_all.at[ep_size - CORES + i, :, chunk[k]]
                    remote(src, dst, dev(chip, other), cross_s, cross_r.at[2 + k])

    def gate_up(k):
        def gather_far(p):
            two = slice(2 * p * cap, 2 * (p + 1) * cap)
            xg[two, chunk[k]] = xg[two, chunk[k]] + dot(p_all[two, n_near:], x_rest[:, :, chunk[k]].reshape(rows - n_near, -1)).astype(BF16)

        gather_far(0)
        for e in range(n_exp):
            if e % 2 == 0 and e + 2 < n_exp:
                gather_far(e // 2 + 1)
            own = slice(e * cap, (e + 1) * cap)
            row = e % 4 * cap
            xe = xg[own, chunk[k]]
            h = []
            for m, w in enumerate((wg, wu)):
                total_h = dot(xe, w[e, chunk[k], :])
                for c in range(2):
                    spot = sbuf.at[4 * m + 2 * c + e // 4, row // (chips * tok), row % (chips * tok) : row % (chips * tok) + cap, :]
                    piece = total_h[:, c * COLS : (c + 1) * COLS]
                    if k == 0:
                        spot[...] = piece
                    else:
                        h.append(spot[...] + piece)
            if k:
                for c in range(2):
                    hbuf[own, c * COLS : (c + 1) * COLS] = (jax.nn.silu(h[c]) * h[2 + c]).astype(BF16)

    gather_near(0)
    pass_far(0)
    gather_near(1)
    pass_far(1)
    with jax.named_scope("farwait0"):
        await_all(x_all.at[0 : chips - 2], cross_r.at[1])
        far_wait(0)
        weights[0].wait()
        weights[1].wait()
    with jax.named_scope("gateup0"):
        gate_up(0)
    with jax.named_scope("farwait1"):
        far_wait(1)
        for copy in weights[2:5]:
            copy.wait()

    part = []

    def last(j):
        cols = slice(j * COLS, (j + 1) * COLS)
        for e in range(n_exp):
            y = dot(hbuf[e * cap : (e + 1) * cap, :], wd[e, :, cols]).astype(BF16)
            for k in range(3):
                ybuf[j % 2, k * pairs + e * cap : k * pairs + (e + 1) * cap, :] = y

    def compute(j):
        if j == 1:
            last(1)
        if j and j + 1 < n_blk:
            last(j + 1)
        for k in range(CORES):
            sbuf[j, k] = dot(acat[k * chips * tok : (k + 1) * chips * tok, :], ybuf[j % 2])
        part.append(remote(sbuf.at[j, 1], d2d.at[j], dev(chip, other), d2d_s, d2d_r.at[j]))

    lo, up = slice(0, hc), slice(hc, COLS)
    half_blk = n_blk // 2

    def send(j):
        part[j].wait_recv()
        tbuf[j] = (sbuf[j, 0] + d2d[j]).reshape(chips, tok, COLS)
        remote(tbuf.at[j, POS_FAR, :, lo], hop.at[j, :, lo], dev(right, core), hop_s, hop_r.at[j])
        remote(tbuf.at[j, POS_FAR, :, up], hop.at[j, :, up], dev(left, core), hop_s, hop_r.at[j])

    def direct(j):
        remote(tbuf.at[j, POS_RIGHT, :, up], froml.at[j, :, up], dev(right, core), dir_s, end_r.at[0, j // half_blk])
        remote(tbuf.at[j, POS_LEFT, :, lo], fromr.at[j, :, lo], dev(left, core), dir_s, end_r.at[1, j // half_blk])

    def relay(j):
        await_all(hop.at[j], hop_r.at[j])
        rel[j, :, lo] = hop[j, :, lo] + tbuf[j, POS_RIGHT, :, lo]
        rel[j, :, up] = hop[j, :, up] + tbuf[j, POS_LEFT, :, up]
        remote(rel.at[j, :, lo], froml.at[j, :, lo], dev(right, core), rel_s, end_r.at[0, j // half_blk])
        remote(rel.at[j, :, up], fromr.at[j, :, up], dev(left, core), rel_s, end_r.at[1, j // half_blk])

    def finish(k):
        blks = slice(k * half_blk, (k + 1) * half_blk)
        await_all(froml.at[blks], end_r.at[0, k])
        await_all(fromr.at[blks], end_r.at[1, k])
        for j in range(k * half_blk, (k + 1) * half_blk):
            cols = slice(j * COLS, (j + 1) * COLS)
            routed = (tbuf[j, POS_OWN] + froml[j]) + fromr[j]
            out_ref[:, cols] = ((hid[:, cols].astype(F32) + shared[:, cols].astype(F32)) + routed).astype(BF16)

    def scoped(f, j):
        with jax.named_scope(f"{f.__name__}{j}"):
            f(j)

    with jax.named_scope("gateup1"):
        gate_up(1)
        last(0)
        compute(0)
    weights[5].wait()
    for j in range(n_blk):
        if j:
            scoped(compute, j)
        if j >= 1:
            scoped(send, j - 1)
            scoped(direct, j - 1)
    scoped(send, n_blk - 1)

    with jax.named_scope("shared"):
        for copy in weights[6:]:
            copy.wait()
        xs = x_all[0]
        mid_cols = hsh.shape[1] // 2

        def shared_part(k):
            cols = slice(k * mid_cols, (k + 1) * mid_cols)
            hsh[:, cols] = (jax.nn.silu(dot(xs, sg[:, cols])) * dot(xs, su[:, cols])).astype(BF16)

        scoped(relay, 0)
        scoped(relay, 1)
        scoped(direct, n_blk - 1)
        shared_part(0)
        scoped(relay, 2)
        scoped(relay, 3)
        shared_part(1)
        scoped(relay, 4)
        scoped(relay, 5)
        shared[...] = dot(hsh[...], sd[...]).astype(BF16)
    for k in range(2):
        scoped(finish, k)
    with jax.named_scope("drain"):
        await_all(x_all.at[0:3], ring_s)
        @pl.when(core == HUB)
        def _():
            await_all(x_all.at[0 : chips + 1], cross_s)

        @pl.when(core != HUB)
        def _():
            await_all(x_all.at[0 : chips - 1], cross_s)

        await_all(gt_send.at[0 : ep_size - 1], tile_s)
        await_all(d2d, d2d_s)
        await_all(hop, hop_s)
        await_all(froml, dir_s)
        await_all(rel, rel_s)


def put_kernel(src, dst, o_sem):
    copy = pltpu.make_async_copy(src, dst, o_sem)
    copy.start()
    copy.wait()


def solution(mesh):
    ep_size = mesh.shape["ep"]

    def local_block(hidden_in, norm_gain, router_w, w_gate, w_up, w_down, ws_gate, ws_up, ws_down, expert_ids):
        tok, top_k = expert_ids.shape
        dim = hidden_in.shape[1]
        n_exp, _, inter = w_gate.shape
        s_inter = ws_gate.shape[1]
        cap = GROUPS * ((top_k + GROUP_LIMIT - 1) // GROUP_LIMIT) * tok // n_exp
        rows = ep_size * tok
        pairs = n_exp * cap
        n_blk = dim // COLS
        chips = ep_size // CORES
        vm, sem = pltpu.VMEM, pltpu.SemaphoreType.DMA
        scratch = [
            vm((tok, dim), BF16), vm((dim // 128, 128), F32), vm(router_w.shape, F32), vm((top_k, tok), jnp.int32),
            vm(w_gate.shape, BF16), vm(w_up.shape, BF16), vm(w_down.shape, BF16),
            vm(ws_gate.shape, BF16), vm(ws_up.shape, BF16), vm(ws_down.shape, BF16),
            vm((ep_size, tok, dim), BF16), vm((ep_size, n_exp, 128), F32), vm((ep_size, n_exp, 128), F32),
            vm((pairs, rows), BF16),
            vm((rows, 3 * pairs), BF16),
            vm((pairs, dim), BF16), vm((pairs, inter), BF16), vm((2, 3 * pairs, COLS), BF16),
            vm((8, CORES, chips * tok, COLS), F32), vm((n_blk, chips * tok, COLS), F32), vm((n_blk, chips, tok, COLS), F32),
            vm((n_blk, tok, COLS), F32), vm((n_blk, tok, COLS), F32), vm((n_blk, tok, COLS), F32), vm((n_blk, tok, COLS), F32),
            vm((tok, s_inter), BF16), vm((tok, dim), BF16),
            sem((4,)), sem((9,)), sem, sem, sem, sem, sem, sem, sem,
            sem((10,)), sem((4,)), sem, sem((n_blk,)), sem((n_blk,)), sem((2, 2)),
        ]
        result = pl.pallas_call(
            functools.partial(moe_kernel, ep_size, cap),
            out_shape=pltpu.VMEM((tok, dim), BF16),
            in_specs=[pl.BlockSpec(memory_space=pl.ANY)] * 10,
            out_specs=pl.BlockSpec(memory_space=pltpu.VMEM),
            scratch_shapes=scratch,
            compiler_params=pltpu.CompilerParams(collective_id=0, has_side_effects=True, vmem_limit_bytes=65_800_000),
            name="moe_block",
        )(hidden_in, norm_gain.reshape(dim // 128, 128), router_w, w_gate, w_up, w_down, ws_gate, ws_up, ws_down, expert_ids.T)
        return result

    row_spec = P(("dp", "ep"), None)
    in_specs = (row_spec, P(), P(), P("ep"), P("ep"), P("ep"), P(), P(), P(), row_spec)
    return jax.shard_map(local_block, mesh=mesh, in_specs=in_specs, out_specs=row_spec, check_vma=False)
```

```python
import functools

import jax
import jax.numpy as jnp
from jax import lax
from jax.experimental import pallas as pl
from jax.experimental.pallas import tpu as pltpu
from jax.sharding import PartitionSpec as P

NORM_EPS = 1e-6
ROUTE_SCALE = 2.5
GROUPS = 8
GROUP_LIMIT = 4
CORES = 2
HUB = 1
S_ROW = (0, 1, 2, 4, 5, 6, 3, 7)
POS_OWN, POS_RIGHT, POS_LEFT, POS_FAR = range(4)
COLS = 256
CHUNK = 512
MESH = pl.DeviceIdType.MESH
F32 = jnp.float32
BF16 = jnp.bfloat16


def dot(a, b):
    return jnp.dot(a, b, preferred_element_type=F32)


def dot_t(a, b):
    return lax.dot_general(a, b, (((1,), (1,)), ((), ())), preferred_element_type=F32)


def split3(v):
    hi = v.astype(BF16)
    rest = v - hi.astype(F32)
    mid = rest.astype(BF16)
    low = (rest - mid.astype(F32)).astype(BF16)
    return hi, mid, low


def moe_kernel(ep_size, cap, hid_h, gain_h, rw_h, wg_h, wu_h, wd_h, sg_h, su_h, sd_h, ids_h, out_ref,
               hid, gain, rw, ids, wg, wu, wd, sg, su, sd, x_all, gt_send, gt_all, p_all, acat,
               xg, hbuf, ybuf, sbuf, d2d, tbuf, hop, rel, froml, fromr, hsh, shared,
               in_sem, w_sem,
               ring_s, cross_s, tile_s, d2d_s, hop_s, dir_s, rel_s, ag_r, cross_r, tile_r, d2d_r, hop_r, end_r):
    chips = ep_size // CORES
    tok, dim = hid.shape
    n_exp, _, inter = wg.shape
    top_k = ids.shape[0]
    half = dim // 2
    rows = ep_size * tok
    n_blk = dim // COLS
    hc = COLS // 2
    pairs = n_exp * cap

    me = lax.axis_index("ep")
    chip, core = me // CORES, me % CORES
    other = 1 - core
    right, left, opp = (chip + 1) % chips, (chip + chips - 1) % chips, (chip + 2) % chips

    def slot(a_chip, a_core, at_chip=chip, at_core=core):
        away = (a_chip - at_chip + chips) % chips
        pos = away + away // 2 - 2 * (away // 3)
        cross_core = (a_core + at_core) % CORES
        is_far = pos // POS_FAR
        return pos + (chips - 1) * cross_core + is_far * (chips - 1 - (chips - 2) * cross_core)

    def dev(a_chip, a_core):
        return {"ep": a_chip * CORES + a_core}

    def remote(src, dst, to, s_sem, r_sem):
        copy = pltpu.make_async_remote_copy(src, dst, s_sem, r_sem, device_id=to, device_id_type=MESH)
        copy.start()
        return copy

    def await_all(ref, sem):
        pltpu.make_async_copy(ref, ref, sem).wait()

    ins = [pltpu.make_async_copy(s, d, in_sem.at[i]) for i, (s, d) in enumerate(((hid_h, hid), (gain_h, gain), (rw_h, rw), (ids_h, ids)))]
    for copy in ins:
        copy.start()
    early, late = slice(0, COLS), slice(COLS, dim)
    chunk = (slice(0, CHUNK), slice(CHUNK, dim))
    fetches = [(h.at[:, rng, :], v.at[:, rng, :]) for rng in chunk for h, v in ((wg_h, wg), (wu_h, wu))]
    fetches += [(wd_h.at[:, :, early], wd.at[:, :, early]), (wd_h.at[:, :, late], wd.at[:, :, late]), (sg_h, sg), (su_h, su), (sd_h, sd)]
    weights = []
    for i, (s, d) in enumerate(fetches):
        weights.append(pltpu.make_async_copy(s, d, w_sem.at[i]))
        weights[-1].start(priority=1)

    barrier = pltpu.get_barrier_semaphore()
    for k in range(1, ep_size):
        pl.semaphore_signal(barrier, inc=1, device_id={"ep": (me + k) % ep_size}, device_id_type=MESH)

    with jax.named_scope("norm"):
        ins[0].wait()
        ins[1].wait()
        x_f32 = hid[...].astype(F32)
        inv_rms = lax.rsqrt(jnp.mean(x_f32 * x_f32, axis=-1, keepdims=True) + NORM_EPS)
        gain_row = jnp.concatenate([gain[i : i + 1, :] for i in range(dim // 128)], axis=1)
        x_norm = (x_f32 * inv_rms * gain_row).astype(BF16)
        x_all[0] = x_norm

    with jax.named_scope("barwait"):
        pl.semaphore_wait(barrier, ep_size - 1)

    side_a = [slice(0, CHUNK // 2), slice(CHUNK, (CHUNK + dim) // 2)]
    side_b = [slice(CHUNK // 2, CHUNK), slice((CHUNK + dim) // 2, dim)]

    def spread(a_chip, cols, to, r_sem, to_core=core):
        src, dst = x_all.at[slot(a_chip, core), :, cols], x_all.at[slot(a_chip, core, to, to_core), :, cols]
        return remote(src, dst, dev(to, to_core), ring_s, r_sem)

    def cross(a_chip, cols, r_sem):
        src, dst = x_all.at[slot(a_chip, core), :, cols], x_all.at[slot(a_chip, core, chip, other), :, cols]
        remote(src, dst, dev(chip, other), cross_s, r_sem)

    ra, lb = [], []
    for k in range(2):
        ra.append(spread(chip, side_a[k], right, ag_r.at[k]))
        lb.append(spread(chip, side_b[k], left, ag_r.at[2 + k]))

    with jax.named_scope("router"):
        ins[2].wait()
        ins[3].wait()
        r_hi, r_mid, r_low = split3(rw[...])
        logits = (dot_t(r_low, x_norm) + dot_t(r_mid, x_norm)) + dot_t(r_hi, x_norm)
        scores = 1.0 / (1.0 + jnp.exp(-logits))
        exp_no = lax.broadcasted_iota(jnp.int32, logits.shape, 0)
        chosen = exp_no == ids[0:1, :]
        for k in range(1, top_k):
            chosen = jnp.logical_or(chosen, exp_no == ids[k : k + 1, :])
        total = jnp.sum(jnp.where(chosen, scores, 0.0), axis=0, keepdims=True)
        gates = jnp.where(chosen, ROUTE_SCALE * scores / total, -1.0)
        gt_send[...] = jnp.full(gt_send.shape, -1.0, F32)
        for d in range(ep_size):
            gt_send[d, :, 0:tok] = gates[d * n_exp : (d + 1) * n_exp, :]
        gt_all[0] = gt_send[me]
        for k in range(1, ep_size):
            to = (me + k) % ep_size
            remote(gt_send.at[to], gt_all.at[slot(chip, core, to // CORES, to % CORES)], {"ep": to}, tile_s, tile_r)

    for k in range(2):
        spread(chip, side_b[k], right, ag_r.at[4 + k])
        spread(chip, side_a[k], left, ag_r.at[4 + k])
    cross(chip, slice(0, dim), cross_r.at[0])

    with jax.named_scope("relays"):
        for k in range(2):
            ra[k].wait_recv()
            spread(left, side_a[k], right, ag_r.at[6 + 2 * k], HUB)
            cross(left, side_a[k], cross_r.at[1 + k])
            lb[k].wait_recv()
            spread(right, side_b[k], left, ag_r.at[7 + 2 * k], HUB)
            cross(right, side_b[k], cross_r.at[1 + k])

    def near_rest(k):
        with jax.named_scope(f"rest{k}"):
            await_all(x_all.at[0, :, chunk[k]], ag_r.at[4 + k])
            cross(left, side_b[k], cross_r.at[1 + k])
            cross(right, side_a[k], cross_r.at[1 + k])

    with jax.named_scope("tilewait"):
        await_all(gt_all.at[0 : ep_size - 1], tile_r)

    with jax.named_scope("onehot"):
        lane_src = lax.broadcasted_iota(jnp.int32, (n_exp, rows), 1) // tok
        gmat = jnp.full((n_exp, rows), -1.0, F32)
        for s in range(ep_size):
            wide = jnp.concatenate([gt_all[s], jnp.full((n_exp, rows - gt_all.shape[2]), -1.0, F32)], axis=1)
            if s:
                wide = pltpu.roll(wide, s * tok, 1)
            gmat = jnp.where(lane_src == s, wide, gmat)
        picked = jnp.logical_not(gmat < 0.0)
        upper = lax.broadcasted_iota(jnp.int32, (rows, rows), 0) < lax.broadcasted_iota(jnp.int32, (rows, rows), 1)
        rank = dot(jnp.where(picked, 1.0, 0.0).astype(BF16), jnp.where(upper, 1.0, 0.0).astype(BF16))
        place = jnp.where(picked, rank, -1.0)
        for i in range(pairs // 128):
            e_one, e_two = i * 128 // cap, (i * 128 + 127) // cap
            row_no = lax.broadcasted_iota(jnp.int32, (128, rows), 0) + i * 128
            first = row_no < e_two * cap
            pos = (row_no - jnp.where(first, e_one * cap, e_two * cap)).astype(F32)
            hit = pos == jnp.where(first, place[e_one : e_one + 1, :], place[e_two : e_two + 1, :])
            gated = jnp.where(hit, jnp.where(first, gmat[e_one : e_one + 1, :], gmat[e_two : e_two + 1, :]), 0.0)
            p_all[i * 128 : (i + 1) * 128, :] = jnp.where(hit, 1.0, 0.0).astype(BF16)
            for k, term in enumerate(reversed(split3(gated.T))):
                for b in range(ep_size):
                    to_row = S_ROW[b] * tok
                    acat[to_row : to_row + tok, k * pairs + i * 128 : k * pairs + (i + 1) * 128] = term[b * tok : (b + 1) * tok, :]

    n_near = rows // 2
    with jax.named_scope("nearwait"):
        await_all(x_all.at[0], cross_r.at[0])
    x_near = x_all.at[0 : ep_size // 2]
    x_rest = x_all.at[ep_size // 2 : ep_size]

    far_slots = slice(ep_size - CORES, ep_size)

    def far_wait(k):
        @pl.when(core != HUB)
        def _():
            await_all(x_all.at[far_slots, :, chunk[k]], cross_r.at[3 + k])

    def gather_near(k):
        with jax.named_scope(f"near{k}"):
            xg[:, chunk[k]] = dot(p_all[:, 0:n_near], x_near[:, :, chunk[k]].reshape(n_near, -1)).astype(BF16)

    def pass_far(k):
        with jax.named_scope(f"far{k}"):
            @pl.when(core == HUB)
            def _():
                for r_sem, cols in ((6 + 2 * k, side_a[k]), (7 + 2 * k, side_b[k])):
                    await_all(x_all.at[far_slots, :, cols], ag_r.at[r_sem])
                for i in range(CORES):
                    src, dst = x_all.at[ep_size - 1 - i, :, chunk[k]], x_all.at[ep_size - CORES + i, :, chunk[k]]
                    remote(src, dst, dev(chip, other), cross_s, cross_r.at[3 + k])

    def gate_up(k):
        def gather_far(p):
            two = slice(2 * p * cap, 2 * (p + 1) * cap)
            xg[two, chunk[k]] = xg[two, chunk[k]] + dot(p_all[two, n_near:], x_rest[:, :, chunk[k]].reshape(rows - n_near, -1)).astype(BF16)

        gather_far(0)
        for e in range(n_exp):
            if e % 2 == 0 and e + 2 < n_exp:
                gather_far(e // 2 + 1)
            own = slice(e * cap, (e + 1) * cap)
            row = e % 4 * cap
            xe = xg[own, chunk[k]]
            h = []
            for m, w in enumerate((wg, wu)):
                total_h = dot(xe, w[e, chunk[k], :])
                for c in range(2):
                    spot = sbuf.at[4 * m + 2 * c + e // 4, row // (chips * tok), row % (chips * tok) : row % (chips * tok) + cap, :]
                    piece = total_h[:, c * COLS : (c + 1) * COLS]
                    if k == 0:
                        spot[...] = piece
                    else:
                        h.append(spot[...] + piece)
            if k:
                for c in range(2):
                    hbuf[own, c * COLS : (c + 1) * COLS] = (jax.nn.silu(h[c]) * h[2 + c]).astype(BF16)

    near_rest(0)
    gather_near(0)
    near_rest(1)
    pass_far(0)
    gather_near(1)
    pass_far(1)
    with jax.named_scope("farwait0"):
        await_all(x_all.at[0 : chips - 2, :, chunk[0]], cross_r.at[1])
        far_wait(0)
        weights[0].wait()
        weights[1].wait()
    with jax.named_scope("gateup0"):
        gate_up(0)
    with jax.named_scope("farwait1"):
        await_all(x_all.at[0 : chips - 2, :, chunk[1]], cross_r.at[2])
        far_wait(1)
        for copy in weights[2:5]:
            copy.wait()

    part = []

    def last(j):
        cols = slice(j * COLS, (j + 1) * COLS)
        for e in range(n_exp):
            y = dot(hbuf[e * cap : (e + 1) * cap, :], wd[e, :, cols]).astype(BF16)
            for k in range(3):
                ybuf[j % 2, k * pairs + e * cap : k * pairs + (e + 1) * cap, :] = y

    def compute(j):
        if j == 1:
            last(1)
        if j and j + 1 < n_blk:
            last(j + 1)
        for k in range(CORES):
            sbuf[j, k] = dot(acat[k * chips * tok : (k + 1) * chips * tok, :], ybuf[j % 2])
        part.append(remote(sbuf.at[j, 1], d2d.at[j], dev(chip, other), d2d_s, d2d_r.at[j]))

    lo, up = slice(0, hc), slice(hc, COLS)
    half_blk = n_blk // 2

    def send(j):
        part[j].wait_recv()
        tbuf[j] = (sbuf[j, 0] + d2d[j]).reshape(chips, tok, COLS)
        remote(tbuf.at[j, POS_FAR, :, lo], hop.at[j, :, lo], dev(right, core), hop_s, hop_r.at[j])
        remote(tbuf.at[j, POS_FAR, :, up], hop.at[j, :, up], dev(left, core), hop_s, hop_r.at[j])

    def direct(j):
        remote(tbuf.at[j, POS_RIGHT, :, up], froml.at[j, :, up], dev(right, core), dir_s, end_r.at[0, j // half_blk])
        remote(tbuf.at[j, POS_LEFT, :, lo], fromr.at[j, :, lo], dev(left, core), dir_s, end_r.at[1, j // half_blk])

    def relay(j):
        await_all(hop.at[j], hop_r.at[j])
        rel[j, :, lo] = hop[j, :, lo] + tbuf[j, POS_RIGHT, :, lo]
        rel[j, :, up] = hop[j, :, up] + tbuf[j, POS_LEFT, :, up]
        remote(rel.at[j, :, lo], froml.at[j, :, lo], dev(right, core), rel_s, end_r.at[0, j // half_blk])
        remote(rel.at[j, :, up], fromr.at[j, :, up], dev(left, core), rel_s, end_r.at[1, j // half_blk])

    def finish(k):
        blks = slice(k * half_blk, (k + 1) * half_blk)
        await_all(froml.at[blks], end_r.at[0, k])
        await_all(fromr.at[blks], end_r.at[1, k])
        for j in range(k * half_blk, (k + 1) * half_blk):
            cols = slice(j * COLS, (j + 1) * COLS)
            routed = (tbuf[j, POS_OWN] + froml[j]) + fromr[j]
            out_ref[:, cols] = ((hid[:, cols].astype(F32) + shared[:, cols].astype(F32)) + routed).astype(BF16)

    def scoped(f, j):
        with jax.named_scope(f"{f.__name__}{j}"):
            f(j)

    with jax.named_scope("gateup1"):
        gate_up(1)
        last(0)
        compute(0)
    weights[5].wait()
    for j in range(n_blk):
        if j:
            scoped(compute, j)
        if j >= 1:
            scoped(send, j - 1)
            scoped(direct, j - 1)
    scoped(send, n_blk - 1)

    with jax.named_scope("shared"):
        for copy in weights[6:]:
            copy.wait()
        xs = x_all[0]
        mid_cols = hsh.shape[1] // 2

        def shared_part(k):
            cols = slice(k * mid_cols, (k + 1) * mid_cols)
            hsh[:, cols] = (jax.nn.silu(dot(xs, sg[:, cols])) * dot(xs, su[:, cols])).astype(BF16)

        scoped(relay, 0)
        scoped(relay, 1)
        scoped(direct, n_blk - 1)
        shared_part(0)
        scoped(relay, 2)
        scoped(relay, 3)
        shared_part(1)
        scoped(relay, 4)
        scoped(relay, 5)
        shared[...] = dot(hsh[...], sd[...]).astype(BF16)
    for k in range(2):
        scoped(finish, k)
    with jax.named_scope("drain"):
        await_all(x_all.at[0:3], ring_s)
        @pl.when(core == HUB)
        def _():
            await_all(x_all.at[0 : chips + 1], cross_s)

        @pl.when(core != HUB)
        def _():
            await_all(x_all.at[0 : chips - 1], cross_s)

        await_all(gt_send.at[0 : ep_size - 1], tile_s)
        await_all(d2d, d2d_s)
        await_all(hop, hop_s)
        await_all(froml, dir_s)
        await_all(rel, rel_s)


def put_kernel(src, dst, o_sem):
    copy = pltpu.make_async_copy(src, dst, o_sem)
    copy.start()
    copy.wait()


def solution(mesh):
    ep_size = mesh.shape["ep"]

    def local_block(hidden_in, norm_gain, router_w, w_gate, w_up, w_down, ws_gate, ws_up, ws_down, expert_ids):
        tok, top_k = expert_ids.shape
        dim = hidden_in.shape[1]
        n_exp, _, inter = w_gate.shape
        s_inter = ws_gate.shape[1]
        cap = GROUPS * ((top_k + GROUP_LIMIT - 1) // GROUP_LIMIT) * tok // n_exp
        rows = ep_size * tok
        pairs = n_exp * cap
        n_blk = dim // COLS
        chips = ep_size // CORES
        vm, sem = pltpu.VMEM, pltpu.SemaphoreType.DMA
        scratch = [
            vm((tok, dim), BF16), vm((dim // 128, 128), F32), vm(router_w.shape, F32), vm((top_k, tok), jnp.int32),
            vm(w_gate.shape, BF16), vm(w_up.shape, BF16), vm(w_down.shape, BF16),
            vm(ws_gate.shape, BF16), vm(ws_up.shape, BF16), vm(ws_down.shape, BF16),
            vm((ep_size, tok, dim), BF16), vm((ep_size, n_exp, 128), F32), vm((ep_size, n_exp, 128), F32),
            vm((pairs, rows), BF16),
            vm((rows, 3 * pairs), BF16),
            vm((pairs, dim), BF16), vm((pairs, inter), BF16), vm((2, 3 * pairs, COLS), BF16),
            vm((8, CORES, chips * tok, COLS), F32), vm((n_blk, chips * tok, COLS), F32), vm((n_blk, chips, tok, COLS), F32),
            vm((n_blk, tok, COLS), F32), vm((n_blk, tok, COLS), F32), vm((n_blk, tok, COLS), F32), vm((n_blk, tok, COLS), F32),
            vm((tok, s_inter), BF16), vm((tok, dim), BF16),
            sem((4,)), sem((9,)), sem, sem, sem, sem, sem, sem, sem,
            sem((10,)), sem((5,)), sem, sem((n_blk,)), sem((n_blk,)), sem((2, 2)),
        ]
        result = pl.pallas_call(
            functools.partial(moe_kernel, ep_size, cap),
            out_shape=pltpu.VMEM((tok, dim), BF16),
            in_specs=[pl.BlockSpec(memory_space=pl.ANY)] * 10,
            out_specs=pl.BlockSpec(memory_space=pltpu.VMEM),
            scratch_shapes=scratch,
            compiler_params=pltpu.CompilerParams(collective_id=0, has_side_effects=True, vmem_limit_bytes=65_800_000),
            name="moe_block",
        )(hidden_in, norm_gain.reshape(dim // 128, 128), router_w, w_gate, w_up, w_down, ws_gate, ws_up, ws_down, expert_ids.T)
        return result

    row_spec = P(("dp", "ep"), None)
    in_specs = (row_spec, P(), P(), P("ep"), P("ep"), P("ep"), P(), P(), P(), row_spec)
    return jax.shard_map(local_block, mesh=mesh, in_specs=in_specs, out_specs=row_spec, check_vma=False)
```

```python
import functools

import jax
import jax.numpy as jnp
from jax import lax
from jax.experimental import pallas as pl
from jax.experimental.pallas import tpu as pltpu
from jax.sharding import PartitionSpec as P

NORM_EPS = 1e-6
ROUTE_SCALE = 2.5
GROUPS = 8
GROUP_LIMIT = 4
CORES = 2
HUB = 1
SPLIT = 4
S_ROW = (0, 1, 2, 4, 5, 6, 3, 7)
POS_OWN, POS_RIGHT, POS_LEFT, POS_FAR = range(4)
COLS = 256
CHUNK = 512
MESH = pl.DeviceIdType.MESH
F32 = jnp.float32
BF16 = jnp.bfloat16


def dot(a, b):
    return jnp.dot(a, b, preferred_element_type=F32)


def dot_t(a, b):
    return lax.dot_general(a, b, (((1,), (1,)), ((), ())), preferred_element_type=F32)


def split3(v):
    hi = v.astype(BF16)
    rest = v - hi.astype(F32)
    mid = rest.astype(BF16)
    low = (rest - mid.astype(F32)).astype(BF16)
    return hi, mid, low


def moe_kernel(ep_size, cap, hid_h, gain_h, rw_h, wg_h, wu_h, wd_h, sg_h, su_h, sd_h, ids_h, out_ref,
               hid, gain, rw, ids, wg, wu, wd, sg, su, sd, x_all, gt_send, gt_all, p_all, acat,
               xg, hbuf, ybuf, sbuf, d2d, tbuf, hop, rel, froml, fromr, hsh, shared,
               in_sem, w_sem,
               ring_s, cross_s, tile_s, d2d_s, ret_s, ag_r, cross_r, tile_r, d2d_r, hop_r, end_r):
    chips = ep_size // CORES
    tok, dim = hid.shape
    n_exp, _, inter = wg.shape
    top_k = ids.shape[0]
    half = dim // 2
    rows = ep_size * tok
    n_blk = dim // COLS
    hc = COLS // 2
    pairs = n_exp * cap

    me = lax.axis_index("ep")
    chip, core = me // CORES, me % CORES
    other = 1 - core
    right, left, opp = (chip + 1) % chips, (chip + chips - 1) % chips, (chip + 2) % chips

    def slot(a_chip, a_core, at_chip=chip, at_core=core):
        away = (a_chip - at_chip + chips) % chips
        pos = away + away // 2 - 2 * (away // 3)
        cross_core = (a_core + at_core) % CORES
        is_far = pos // POS_FAR
        return pos + (chips - 1) * cross_core + is_far * (chips - 1 - (chips - 2) * cross_core)

    def dev(a_chip, a_core):
        return {"ep": a_chip * CORES + a_core}

    def remote(src, dst, to, s_sem, r_sem):
        copy = pltpu.make_async_remote_copy(src, dst, s_sem, r_sem, device_id=to, device_id_type=MESH)
        copy.start()
        return copy

    def await_all(ref, sem):
        pltpu.make_async_copy(ref, ref, sem).wait()

    ins = [pltpu.make_async_copy(s, d, in_sem.at[i]) for i, (s, d) in enumerate(((hid_h, hid), (gain_h, gain), (rw_h, rw), (ids_h, ids)))]
    for copy in ins:
        copy.start()
    early, late = slice(0, COLS), slice(COLS, dim)
    chunk = (slice(0, CHUNK), slice(CHUNK, dim))
    fetches = [(h.at[:, rng, :], v.at[:, rng, :]) for rng in chunk for h, v in ((wg_h, wg), (wu_h, wu))]
    fetches += [(wd_h.at[:, :, early], wd.at[:, :, early]), (wd_h.at[:, :, late], wd.at[:, :, late]), (sg_h, sg), (su_h, su), (sd_h, sd)]
    weights = []
    for i, (s, d) in enumerate(fetches):
        weights.append(pltpu.make_async_copy(s, d, w_sem.at[min(i, 6)]))
        weights[-1].start(priority=1)

    barrier = pltpu.get_barrier_semaphore()
    for k in range(1, ep_size):
        pl.semaphore_signal(barrier, inc=1, device_id={"ep": (me + k) % ep_size}, device_id_type=MESH)

    with jax.named_scope("norm"):
        ins[0].wait()
        ins[1].wait()
        x_f32 = hid[...].astype(F32)
        inv_rms = lax.rsqrt(jnp.mean(x_f32 * x_f32, axis=-1, keepdims=True) + NORM_EPS)
        gain_row = jnp.concatenate([gain[i : i + 1, :] for i in range(dim // 128)], axis=1)
        x_norm = (x_f32 * inv_rms * gain_row).astype(BF16)
        x_all[0] = x_norm

    with jax.named_scope("barwait"):
        pl.semaphore_wait(barrier, ep_size - 1)

    side_a = [slice(0, CHUNK // 2), slice(CHUNK, (CHUNK + dim) // 2)]
    side_b = [slice(CHUNK // 2, CHUNK), slice((CHUNK + dim) // 2, dim)]

    def spread(a_chip, cols, to, r_sem, to_core=core):
        src, dst = x_all.at[slot(a_chip, core), :, cols], x_all.at[slot(a_chip, core, to, to_core), :, cols]
        return remote(src, dst, dev(to, to_core), ring_s, r_sem)

    def cross(a_chip, cols, r_sem):
        src, dst = x_all.at[slot(a_chip, core), :, cols], x_all.at[slot(a_chip, core, chip, other), :, cols]
        remote(src, dst, dev(chip, other), cross_s, r_sem)

    ra, lb = [], []

    def own_rows(k):
        ra.append(spread(chip, side_a[k], right, ag_r.at[k]))
        lb.append(spread(chip, side_b[k], left, ag_r.at[2 + k]))
        spread(chip, side_b[k], right, ag_r.at[4 + k])
        spread(chip, side_a[k], left, ag_r.at[4 + k])

    own_rows(0)
    cross(chip, slice(0, dim), cross_r.at[0])

    with jax.named_scope("router"):
        ins[2].wait()
        ins[3].wait()
        r_hi, r_mid, r_low = split3(rw[...])
        logits = (dot_t(r_low, x_norm) + dot_t(r_mid, x_norm)) + dot_t(r_hi, x_norm)
        scores = 1.0 / (1.0 + jnp.exp(-logits))
        exp_no = lax.broadcasted_iota(jnp.int32, logits.shape, 0)
        chosen = exp_no == ids[0:1, :]
        for k in range(1, top_k):
            chosen = jnp.logical_or(chosen, exp_no == ids[k : k + 1, :])
        total = jnp.sum(jnp.where(chosen, scores, 0.0), axis=0, keepdims=True)
        gates = jnp.where(chosen, ROUTE_SCALE * scores / total, -1.0)
        gt_send[...] = jnp.full(gt_send.shape, -1.0, F32)
        for d in range(ep_size):
            gt_send[d, :, 0:tok] = gates[d * n_exp : (d + 1) * n_exp, :]
        gt_all[0] = gt_send[me]
        for k in range(1, ep_size):
            to = (me + k) % ep_size
            remote(gt_send.at[to], gt_all.at[slot(chip, core, to // CORES, to % CORES)], {"ep": to}, tile_s, tile_r)

    own_rows(1)

    def pass_on(k):
        with jax.named_scope(f"relays{k}"):
            ra[k].wait_recv()
            spread(left, side_a[k], right, ag_r.at[6 + k], HUB)
            cross(left, side_a[k], cross_r.at[1 + k])
            lb[k].wait_recv()
            spread(right, side_b[k], left, ag_r.at[6 + k], HUB)
            cross(right, side_b[k], cross_r.at[1 + k])

    pass_on(0)

    def near_rest(k):
        with jax.named_scope(f"rest{k}"):
            await_all(x_all.at[0, :, chunk[k]], ag_r.at[4 + k])
            cross(left, side_b[k], cross_r.at[1 + k])
            cross(right, side_a[k], cross_r.at[1 + k])

    with jax.named_scope("tilewait"):
        await_all(gt_all.at[0 : ep_size - 1], tile_r)

    with jax.named_scope("onehot"):
        lane_src = lax.broadcasted_iota(jnp.int32, (n_exp, rows), 1) // tok
        gmat = jnp.full((n_exp, rows), -1.0, F32)
        for s in range(ep_size):
            wide = jnp.concatenate([gt_all[s], jnp.full((n_exp, rows - gt_all.shape[2]), -1.0, F32)], axis=1)
            if s:
                wide = pltpu.roll(wide, s * tok, 1)
            gmat = jnp.where(lane_src == s, wide, gmat)
        picked = jnp.logical_not(gmat < 0.0)
        upper = lax.broadcasted_iota(jnp.int32, (rows, rows), 0) < lax.broadcasted_iota(jnp.int32, (rows, rows), 1)
        rank = dot(jnp.where(picked, 1.0, 0.0).astype(BF16), jnp.where(upper, 1.0, 0.0).astype(BF16))
        place = jnp.where(picked, rank, -1.0)
        for i in range(pairs // 128):
            e_one, e_two = i * 128 // cap, (i * 128 + 127) // cap
            row_no = lax.broadcasted_iota(jnp.int32, (128, rows), 0) + i * 128
            first = row_no < e_two * cap
            pos = (row_no - jnp.where(first, e_one * cap, e_two * cap)).astype(F32)
            hit = pos == jnp.where(first, place[e_one : e_one + 1, :], place[e_two : e_two + 1, :])
            gated = jnp.where(hit, jnp.where(first, gmat[e_one : e_one + 1, :], gmat[e_two : e_two + 1, :]), 0.0)
            p_all[i * 128 : (i + 1) * 128, :] = jnp.where(hit, 1.0, 0.0).astype(BF16)
            for k, term in enumerate(reversed(split3(gated.T))):
                for b in range(ep_size):
                    to_row = S_ROW[b] * tok
                    acat[to_row : to_row + tok, k * pairs + i * 128 : k * pairs + (i + 1) * 128] = term[b * tok : (b + 1) * tok, :]

    n_near = rows // 2
    with jax.named_scope("nearwait"):
        await_all(x_all.at[0], cross_r.at[0])
    x_near = x_all.at[0 : ep_size // 2]
    x_rest = x_all.at[ep_size // 2 : ep_size]

    far_slots = slice(ep_size - CORES, ep_size)

    def far_wait(k):
        @pl.when(core != HUB)
        def _():
            await_all(x_all.at[far_slots, :, chunk[k]], cross_r.at[3 + k])

    def gather_near(k):
        with jax.named_scope(f"near{k}"):
            xg[:, chunk[k]] = dot(p_all[:, 0:n_near], x_near[:, :, chunk[k]].reshape(n_near, -1)).astype(BF16)

    def pass_far(k):
        with jax.named_scope(f"far{k}"):
            @pl.when(core == HUB)
            def _():
                await_all(x_all.at[far_slots, :, chunk[k]], ag_r.at[6 + k])
                for i in range(CORES):
                    src, dst = x_all.at[ep_size - 1 - i, :, chunk[k]], x_all.at[ep_size - CORES + i, :, chunk[k]]
                    remote(src, dst, dev(chip, other), cross_s, cross_r.at[3 + k])

    def gate_up(k, first, end):
        def gather_far(p):
            two = slice(2 * p * cap, 2 * (p + 1) * cap)
            xg[two, chunk[k]] = xg[two, chunk[k]] + dot(p_all[two, n_near:], x_rest[:, :, chunk[k]].reshape(rows - n_near, -1)).astype(BF16)

        gather_far(first // 2)
        for e in range(first, end):
            if e % 2 == 0 and e + 2 < end:
                gather_far(e // 2 + 1)
            own = slice(e * cap, (e + 1) * cap)
            row = e % 4 * cap
            xe = xg[own, chunk[k]]
            h = []
            for m, w in enumerate((wg, wu)):
                total_h = dot(xe, w[e, chunk[k], :])
                for c in range(2):
                    spot = sbuf.at[4 * m + 2 * c + e // 4, row // (chips * tok), row % (chips * tok) : row % (chips * tok) + cap, :]
                    piece = total_h[:, c * COLS : (c + 1) * COLS]
                    if k == 0:
                        spot[...] = piece
                    else:
                        h.append(spot[...] + piece)
            if k:
                for c in range(2):
                    hbuf[own, c * COLS : (c + 1) * COLS] = (jax.nn.silu(h[c]) * h[2 + c]).astype(BF16)

    pass_on(1)
    near_rest(0)
    gather_near(0)
    near_rest(1)
    pass_far(0)
    gather_near(1)
    with jax.named_scope("farwait0"):
        await_all(x_all.at[0 : chips - 2, :, chunk[0]], cross_r.at[1])
        far_wait(0)
        weights[0].wait()
        weights[1].wait()
    with jax.named_scope("gateup0"):
        gate_up(0, 0, SPLIT)
    pass_far(1)
    with jax.named_scope("gateup0b"):
        gate_up(0, SPLIT, n_exp)
    with jax.named_scope("farwait1"):
        await_all(x_all.at[0 : chips - 2, :, chunk[1]], cross_r.at[2])
        far_wait(1)
        for copy in weights[2:5]:
            copy.wait()

    part = []

    def last(j):
        cols = slice(j * COLS, (j + 1) * COLS)
        for e in range(n_exp):
            y = dot(hbuf[e * cap : (e + 1) * cap, :], wd[e, :, cols]).astype(BF16)
            for k in range(3):
                ybuf[j % 2, k * pairs + e * cap : k * pairs + (e + 1) * cap, :] = y

    def compute(j):
        if j == 1:
            last(1)
        if j and j + 1 < n_blk:
            last(j + 1)
        for k in range(CORES):
            sbuf[j, k] = dot(acat[k * chips * tok : (k + 1) * chips * tok, :], ybuf[j % 2])
        part.append(remote(sbuf.at[j, 1], d2d.at[j], dev(chip, other), d2d_s, d2d_r.at[j]))

    lo, up = slice(0, hc), slice(hc, COLS)
    late_blk = n_blk - 1

    def send(j):
        part[j].wait_recv()
        tbuf[j] = (sbuf[j, 0] + d2d[j]).reshape(chips, tok, COLS)
        remote(tbuf.at[j, POS_FAR, :, lo], hop.at[j, :, lo], dev(right, core), ret_s, hop_r.at[j])
        remote(tbuf.at[j, POS_FAR, :, up], hop.at[j, :, up], dev(left, core), ret_s, hop_r.at[j])

    def direct(j):
        remote(tbuf.at[j, POS_RIGHT, :, up], froml.at[j, :, up], dev(right, core), ret_s, end_r.at[j // late_blk])
        remote(tbuf.at[j, POS_LEFT, :, lo], fromr.at[j, :, lo], dev(left, core), ret_s, end_r.at[j // late_blk])

    def relay(j):
        await_all(hop.at[j], hop_r.at[j])
        rel[j, :, lo] = hop[j, :, lo] + tbuf[j, POS_RIGHT, :, lo]
        rel[j, :, up] = hop[j, :, up] + tbuf[j, POS_LEFT, :, up]
        remote(rel.at[j, :, lo], froml.at[j, :, lo], dev(right, core), ret_s, end_r.at[j // late_blk])
        remote(rel.at[j, :, up], fromr.at[j, :, up], dev(left, core), ret_s, end_r.at[j // late_blk])

    def finish(k):
        blks = range(late_blk) if k == 0 else range(late_blk, n_blk)
        await_all(tbuf.at[blks[0] : blks[-1] + 1, 0:2], end_r.at[k])
        for j in blks:
            cols = slice(j * COLS, (j + 1) * COLS)
            routed = (tbuf[j, POS_OWN] + froml[j]) + fromr[j]
            out_ref[:, cols] = ((hid[:, cols].astype(F32) + shared[:, cols].astype(F32)) + routed).astype(BF16)

    def scoped(f, j):
        with jax.named_scope(f"{f.__name__}{j}"):
            f(j)

    with jax.named_scope("gateup1"):
        gate_up(1, 0, n_exp)
        last(0)
        compute(0)
    weights[5].wait()
    for j in range(n_blk):
        if j:
            scoped(compute, j)
        if j >= 1:
            scoped(send, j - 1)
            scoped(direct, j - 1)
    scoped(send, n_blk - 1)

    with jax.named_scope("shared"):
        await_all(wg.at[0 : 3 * sd.shape[0] // inter], w_sem.at[6])
        xs = x_all[0]
        mid_cols = hsh.shape[1] // 2

        def shared_part(k):
            cols = slice(k * mid_cols, (k + 1) * mid_cols)
            hsh[:, cols] = (jax.nn.silu(dot(xs, sg[:, cols])) * dot(xs, su[:, cols])).astype(BF16)

        scoped(relay, 0)
        scoped(relay, 1)
        scoped(direct, n_blk - 1)
        shared_part(0)
        scoped(relay, 2)
        scoped(relay, 3)
        shared_part(1)
        scoped(relay, 4)
        scoped(relay, 5)
        shared[...] = dot(hsh[...], sd[...]).astype(BF16)
    for k in range(2):
        scoped(finish, k)
    with jax.named_scope("drain"):
        await_all(x_all.at[0:3], ring_s)
        @pl.when(core == HUB)
        def _():
            await_all(x_all.at[0 : chips + 1], cross_s)

        @pl.when(core != HUB)
        def _():
            await_all(x_all.at[0 : chips - 1], cross_s)

        await_all(gt_send.at[0 : ep_size - 1], tile_s)
        await_all(d2d, d2d_s)
        await_all(tbuf.at[:, 0:3], ret_s)


def put_kernel(src, dst, o_sem):
    copy = pltpu.make_async_copy(src, dst, o_sem)
    copy.start()
    copy.wait()


def solution(mesh):
    ep_size = mesh.shape["ep"]

    def local_block(hidden_in, norm_gain, router_w, w_gate, w_up, w_down, ws_gate, ws_up, ws_down, expert_ids):
        tok, top_k = expert_ids.shape
        dim = hidden_in.shape[1]
        n_exp, _, inter = w_gate.shape
        s_inter = ws_gate.shape[1]
        cap = GROUPS * ((top_k + GROUP_LIMIT - 1) // GROUP_LIMIT) * tok // n_exp
        rows = ep_size * tok
        pairs = n_exp * cap
        n_blk = dim // COLS
        chips = ep_size // CORES
        vm, sem = pltpu.VMEM, pltpu.SemaphoreType.DMA
        scratch = [
            vm((tok, dim), BF16), vm((dim // 128, 128), F32), vm(router_w.shape, F32), vm((top_k, tok), jnp.int32),
            vm(w_gate.shape, BF16), vm(w_up.shape, BF16), vm(w_down.shape, BF16),
            vm(ws_gate.shape, BF16), vm(ws_up.shape, BF16), vm(ws_down.shape, BF16),
            vm((ep_size, tok, dim), BF16), vm((ep_size, n_exp, 128), F32), vm((ep_size, n_exp, 128), F32),
            vm((pairs, rows), BF16),
            vm((rows, 3 * pairs), BF16),
            vm((pairs, dim), BF16), vm((pairs, inter), BF16), vm((2, 3 * pairs, COLS), BF16),
            vm((8, CORES, chips * tok, COLS), F32), vm((n_blk, chips * tok, COLS), F32), vm((n_blk, chips, tok, COLS), F32),
            vm((n_blk, tok, COLS), F32), vm((n_blk, tok, COLS), F32), vm((n_blk, tok, COLS), F32), vm((n_blk, tok, COLS), F32),
            vm((tok, s_inter), BF16), vm((tok, dim), BF16),
            sem((4,)), sem((7,)), sem, sem, sem, sem, sem,
            sem((8,)), sem((5,)), sem, sem((n_blk,)), sem((n_blk,)), sem((2,)),
        ]
        result = pl.pallas_call(
            functools.partial(moe_kernel, ep_size, cap),
            out_shape=pltpu.VMEM((tok, dim), BF16),
            in_specs=[pl.BlockSpec(memory_space=pl.ANY)] * 10,
            out_specs=pl.BlockSpec(memory_space=pltpu.VMEM),
            scratch_shapes=scratch,
            compiler_params=pltpu.CompilerParams(collective_id=0, has_side_effects=True, vmem_limit_bytes=65_800_000),
            name="moe_block",
        )(hidden_in, norm_gain.reshape(dim // 128, 128), router_w, w_gate, w_up, w_down, ws_gate, ws_up, ws_down, expert_ids.T)
        return result

    row_spec = P(("dp", "ep"), None)
    in_specs = (row_spec, P(), P(), P("ep"), P("ep"), P("ep"), P(), P(), P(), row_spec)
    return jax.shard_map(local_block, mesh=mesh, in_specs=in_specs, out_specs=row_spec, check_vma=False)
```

```python
import functools

import jax
import jax.numpy as jnp
from jax import lax
from jax.experimental import pallas as pl
from jax.experimental.pallas import tpu as pltpu
from jax.sharding import PartitionSpec as P

NORM_EPS = 1e-6
ROUTE_SCALE = 2.5
GROUPS = 8
GROUP_LIMIT = 4
CORES = 2
HUB = 1
SPLIT = 4
S_ROW = (0, 1, 2, 4, 5, 6, 3, 7)
POS_OWN, POS_RIGHT, POS_LEFT, POS_FAR = range(4)
COLS = 256
CHUNK = 512
MESH = pl.DeviceIdType.MESH
F32 = jnp.float32
BF16 = jnp.bfloat16


def dot(a, b):
    return jnp.dot(a, b, preferred_element_type=F32)


def dot_t(a, b):
    return lax.dot_general(a, b, (((1,), (1,)), ((), ())), preferred_element_type=F32)


def split3(v):
    hi = v.astype(BF16)
    rest = v - hi.astype(F32)
    mid = rest.astype(BF16)
    low = (rest - mid.astype(F32)).astype(BF16)
    return hi, mid, low


def moe_kernel(ep_size, cap, hid_h, gain_h, rw_h, wg_h, wu_h, wd_h, sg_h, su_h, sd_h, ids_h, out_ref,
               hid, gain, rw, ids, wg, wu, wd, sg, su, sd, x_all, gt_send, gt_all, p_all, acat,
               xg, hbuf, ybuf, sbuf, d2d, tbuf, hop, rel, froml, fromr, hsh, shared,
               in_sem, w_sem,
               ring_s, cross_s, tile_s, d2d_s, ret_s, ag_r, cross_r, tile_r, d2d_r, hop_r, end_r):
    chips = ep_size // CORES
    tok, dim = hid.shape
    n_exp, _, inter = wg.shape
    top_k = ids.shape[0]
    half = dim // 2
    rows = ep_size * tok
    n_blk = dim // COLS
    hc = COLS // 2
    pairs = n_exp * cap

    me = lax.axis_index("ep")
    chip, core = me // CORES, me % CORES
    other = 1 - core
    right, left, opp = (chip + 1) % chips, (chip + chips - 1) % chips, (chip + 2) % chips

    def slot(a_chip, a_core, at_chip=chip, at_core=core):
        away = (a_chip - at_chip + chips) % chips
        pos = away + away // 2 - 2 * (away // 3)
        cross_core = (a_core + at_core) % CORES
        is_far = pos // POS_FAR
        return pos + (chips - 1) * cross_core + is_far * (chips - 1 - (chips - 2) * cross_core)

    def dev(a_chip, a_core):
        return {"ep": a_chip * CORES + a_core}

    def remote(src, dst, to, s_sem, r_sem):
        copy = pltpu.make_async_remote_copy(src, dst, s_sem, r_sem, device_id=to, device_id_type=MESH)
        copy.start()
        return copy

    def await_all(ref, sem):
        pltpu.make_async_copy(ref, ref, sem).wait()

    ins = [pltpu.make_async_copy(s, d, in_sem.at[i]) for i, (s, d) in enumerate(((hid_h, hid), (gain_h, gain), (rw_h, rw), (ids_h, ids)))]
    for copy in ins:
        copy.start()
    early, late = slice(0, COLS), slice(COLS, dim)
    chunk = (slice(0, CHUNK), slice(CHUNK, dim))
    fetches = [(h.at[:, rng, :], v.at[:, rng, :]) for rng in chunk for h, v in ((wg_h, wg), (wu_h, wu))]
    fetches += [(wd_h.at[:, :, early], wd.at[:, :, early]), (wd_h.at[:, :, late], wd.at[:, :, late]), (sg_h, sg), (su_h, su), (sd_h, sd)]
    weights = []
    for i, (s, d) in enumerate(fetches):
        weights.append(pltpu.make_async_copy(s, d, w_sem.at[min(i, 6)]))
        weights[-1].start(priority=1)

    barrier = pltpu.get_barrier_semaphore()
    for k in range(1, ep_size):
        pl.semaphore_signal(barrier, inc=1, device_id={"ep": (me + k) % ep_size}, device_id_type=MESH)

    with jax.named_scope("norm"):
        ins[0].wait()
        ins[1].wait()
        x_f32 = hid[...].astype(F32)
        inv_rms = lax.rsqrt(jnp.mean(x_f32 * x_f32, axis=-1, keepdims=True) + NORM_EPS)
        gain_row = jnp.concatenate([gain[i : i + 1, :] for i in range(dim // 128)], axis=1)
        x_norm = (x_f32 * inv_rms * gain_row).astype(BF16)
        x_all[0] = x_norm

    with jax.named_scope("barwait"):
        pl.semaphore_wait(barrier, ep_size - 1)

    side_a = [slice(0, CHUNK // 2), slice(CHUNK, (CHUNK + dim) // 2)]
    side_b = [slice(CHUNK // 2, CHUNK), slice((CHUNK + dim) // 2, dim)]

    def spread(a_chip, cols, to, r_sem, to_core=core):
        src, dst = x_all.at[slot(a_chip, core), :, cols], x_all.at[slot(a_chip, core, to, to_core), :, cols]
        return remote(src, dst, dev(to, to_core), ring_s, r_sem)

    def cross(a_chip, cols, r_sem):
        src, dst = x_all.at[slot(a_chip, core), :, cols], x_all.at[slot(a_chip, core, chip, other), :, cols]
        remote(src, dst, dev(chip, other), cross_s, r_sem)

    ra, lb = [], []

    def own_rows(k):
        ra.append(spread(chip, side_a[k], right, ag_r.at[k]))
        lb.append(spread(chip, side_b[k], left, ag_r.at[2 + k]))
        spread(chip, side_b[k], right, ag_r.at[4 + k])
        spread(chip, side_a[k], left, ag_r.at[4 + k])

    own_rows(0)
    cross(chip, slice(0, dim), cross_r.at[0])

    with jax.named_scope("router"):
        ins[2].wait()
        ins[3].wait()
        r_hi, r_mid, r_low = split3(rw[...])
        logits = (dot_t(r_low, x_norm) + dot_t(r_mid, x_norm)) + dot_t(r_hi, x_norm)
        scores = 1.0 / (1.0 + jnp.exp(-logits))
        exp_no = lax.broadcasted_iota(jnp.int32, logits.shape, 0)
        chosen = exp_no == ids[0:1, :]
        for k in range(1, top_k):
            chosen = jnp.logical_or(chosen, exp_no == ids[k : k + 1, :])
        total = jnp.sum(jnp.where(chosen, scores, 0.0), axis=0, keepdims=True)
        gates = jnp.where(chosen, ROUTE_SCALE * scores / total, -1.0)
        gt_send[...] = jnp.full(gt_send.shape, -1.0, F32)
        for d in range(ep_size):
            gt_send[d, :, 0:tok] = gates[d * n_exp : (d + 1) * n_exp, :]
        gt_all[0] = gt_send[me]
        for k in range(1, ep_size):
            to = (me + k) % ep_size
            remote(gt_send.at[to], gt_all.at[slot(chip, core, to // CORES, to % CORES)], {"ep": to}, tile_s, tile_r)

    own_rows(1)

    def pass_on(k):
        with jax.named_scope(f"relays{k}"):
            ra[k].wait_recv()
            spread(left, side_a[k], right, ag_r.at[6 + k], HUB)
            cross(left, side_a[k], cross_r.at[1 + k])
            lb[k].wait_recv()
            spread(right, side_b[k], left, ag_r.at[6 + k], HUB)
            cross(right, side_b[k], cross_r.at[1 + k])

    pass_on(0)

    def near_rest(k):
        with jax.named_scope(f"rest{k}"):
            await_all(x_all.at[0, :, chunk[k]], ag_r.at[4 + k])
            cross(left, side_b[k], cross_r.at[1 + k])
            cross(right, side_a[k], cross_r.at[1 + k])

    with jax.named_scope("tilewait"):
        await_all(gt_all.at[0 : ep_size - 1], tile_r)

    with jax.named_scope("onehot"):
        lane_src = lax.broadcasted_iota(jnp.int32, (n_exp, rows), 1) // tok
        gmat = jnp.full((n_exp, rows), -1.0, F32)
        for s in range(ep_size):
            wide = jnp.concatenate([gt_all[s], jnp.full((n_exp, rows - gt_all.shape[2]), -1.0, F32)], axis=1)
            if s:
                wide = pltpu.roll(wide, s * tok, 1)
            gmat = jnp.where(lane_src == s, wide, gmat)
        picked = jnp.logical_not(gmat < 0.0)
        upper = lax.broadcasted_iota(jnp.int32, (rows, rows), 0) < lax.broadcasted_iota(jnp.int32, (rows, rows), 1)
        rank = dot(jnp.where(picked, 1.0, 0.0).astype(BF16), jnp.where(upper, 1.0, 0.0).astype(BF16))
        place = jnp.where(picked, rank, -1.0)
        for i in range(pairs // 128):
            e_one, e_two = i * 128 // cap, (i * 128 + 127) // cap
            row_no = lax.broadcasted_iota(jnp.int32, (128, rows), 0) + i * 128
            first = row_no < e_two * cap
            pos = (row_no - jnp.where(first, e_one * cap, e_two * cap)).astype(F32)
            hit = pos == jnp.where(first, place[e_one : e_one + 1, :], place[e_two : e_two + 1, :])
            gated = jnp.where(hit, jnp.where(first, gmat[e_one : e_one + 1, :], gmat[e_two : e_two + 1, :]), 0.0)
            p_all[i * 128 : (i + 1) * 128, :] = jnp.where(hit, 1.0, 0.0).astype(BF16)
            for k, term in enumerate(reversed(split3(gated.T))):
                for b in range(ep_size):
                    to_row = S_ROW[b] * tok
                    acat[to_row : to_row + tok, k * pairs + i * 128 : k * pairs + (i + 1) * 128] = term[b * tok : (b + 1) * tok, :]

    n_near = rows // 2
    with jax.named_scope("nearwait"):
        await_all(x_all.at[0], cross_r.at[0])
    x_near = x_all.at[0 : ep_size // 2]
    x_rest = x_all.at[ep_size // 2 : ep_size]

    far_slots = slice(ep_size - CORES, ep_size)

    def far_wait(k):
        @pl.when(core != HUB)
        def _():
            await_all(x_all.at[far_slots, :, chunk[k]], cross_r.at[3 + k])

    def gather_near(k):
        with jax.named_scope(f"near{k}"):
            xg[:, chunk[k]] = dot(p_all[:, 0:n_near], x_near[:, :, chunk[k]].reshape(n_near, -1)).astype(BF16)

    def pass_far(k):
        with jax.named_scope(f"far{k}"):
            @pl.when(core == HUB)
            def _():
                await_all(x_all.at[far_slots, :, chunk[k]], ag_r.at[6 + k])
                for i in range(CORES):
                    src, dst = x_all.at[ep_size - 1 - i, :, chunk[k]], x_all.at[ep_size - CORES + i, :, chunk[k]]
                    remote(src, dst, dev(chip, other), cross_s, cross_r.at[3 + k])

    def gate_up(k, first, end):
        def gather_far(p):
            two = slice(2 * p * cap, 2 * (p + 1) * cap)
            xg[two, chunk[k]] = xg[two, chunk[k]] + dot(p_all[two, n_near:], x_rest[:, :, chunk[k]].reshape(rows - n_near, -1)).astype(BF16)

        gather_far(first // 2)
        for e in range(first, end):
            if e % 2 == 0 and e + 2 < end:
                gather_far(e // 2 + 1)
            own = slice(e * cap, (e + 1) * cap)
            row = e % 4 * cap
            xe = xg[own, chunk[k]]
            h = []
            for m, w in enumerate((wg, wu)):
                total_h = dot(xe, w[e, chunk[k], :])
                for c in range(2):
                    spot = sbuf.at[4 * m + 2 * c + e // 4, row // (chips * tok), row % (chips * tok) : row % (chips * tok) + cap, :]
                    piece = total_h[:, c * COLS : (c + 1) * COLS]
                    if k == 0:
                        spot[...] = piece
                    else:
                        h.append(spot[...] + piece)
            if k:
                for c in range(2):
                    hbuf[own, c * COLS : (c + 1) * COLS] = (jax.nn.silu(h[c]) * h[2 + c]).astype(BF16)

    pass_on(1)
    near_rest(0)
    gather_near(0)
    near_rest(1)
    pass_far(0)
    gather_near(1)
    with jax.named_scope("farwait0"):
        await_all(x_all.at[0 : chips - 2, :, chunk[0]], cross_r.at[1])
        far_wait(0)
        weights[0].wait()
        weights[1].wait()
    with jax.named_scope("gateup0"):
        gate_up(0, 0, SPLIT)
    pass_far(1)
    with jax.named_scope("gateup0b"):
        gate_up(0, SPLIT, n_exp)
    with jax.named_scope("farwait1"):
        await_all(x_all.at[0 : chips - 2, :, chunk[1]], cross_r.at[2])
        far_wait(1)
        for copy in weights[2:5]:
            copy.wait()

    part = []

    def last(j):
        cols = slice(j * COLS, (j + 1) * COLS)
        for e in range(n_exp):
            y = dot(hbuf[e * cap : (e + 1) * cap, :], wd[e, :, cols]).astype(BF16)
            for k in range(3):
                ybuf[j % 2, k * pairs + e * cap : k * pairs + (e + 1) * cap, :] = y

    def compute(j):
        if j == 1:
            last(1)
        if j and j + 1 < n_blk:
            last(j + 1)
        for k in range(CORES):
            sbuf[j, k] = dot(acat[k * chips * tok : (k + 1) * chips * tok, :], ybuf[j % 2])
        part.append(remote(sbuf.at[j, 1], d2d.at[j], dev(chip, other), d2d_s, d2d_r.at[j]))

    lo, up = slice(0, hc), slice(hc, COLS)
    late_blk = n_blk - 1

    def send(j):
        part[j].wait_recv()
        tbuf[j] = (sbuf[j, 0] + d2d[j]).reshape(chips, tok, COLS)
        remote(tbuf.at[j, POS_FAR, :, lo], hop.at[j, :, lo], dev(right, core), ret_s, hop_r.at[j])
        remote(tbuf.at[j, POS_FAR, :, up], hop.at[j, :, up], dev(left, core), ret_s, hop_r.at[j])

    def direct(j):
        remote(tbuf.at[j, POS_RIGHT, :, up], froml.at[j, :, up], dev(right, core), ret_s, end_r.at[j // late_blk])
        remote(tbuf.at[j, POS_LEFT, :, lo], fromr.at[j, :, lo], dev(left, core), ret_s, end_r.at[j // late_blk])

    def relay(j):
        await_all(hop.at[j], hop_r.at[j])
        rel[j, :, lo] = hop[j, :, lo] + tbuf[j, POS_RIGHT, :, lo]
        rel[j, :, up] = hop[j, :, up] + tbuf[j, POS_LEFT, :, up]
        remote(rel.at[j, :, lo], froml.at[j, :, lo], dev(right, core), ret_s, end_r.at[j // late_blk])
        remote(rel.at[j, :, up], fromr.at[j, :, up], dev(left, core), ret_s, end_r.at[j // late_blk])

    def finish(k):
        blks = range(late_blk) if k == 0 else range(late_blk, n_blk)
        await_all(tbuf.at[blks[0] : blks[-1] + 1, 0:2], end_r.at[k])
        for j in blks:
            cols = slice(j * COLS, (j + 1) * COLS)
            routed = (tbuf[j, POS_OWN] + froml[j]) + fromr[j]
            out_ref[:, cols] = ((hid[:, cols].astype(F32) + shared[:, cols].astype(F32)) + routed).astype(BF16)

    def scoped(f, j):
        with jax.named_scope(f"{f.__name__}{j}"):
            f(j)

    with jax.named_scope("gateup1"):
        gate_up(1, 0, n_exp)
        last(0)
        compute(0)
    weights[5].wait()
    for j in range(n_blk):
        if j:
            scoped(compute, j)
        if j >= 1:
            scoped(send, j - 1)
            scoped(direct, j - 1)
    scoped(send, n_blk - 1)

    with jax.named_scope("shared"):
        await_all(wg.at[0 : 3 * sd.shape[0] // inter], w_sem.at[6])
        xs = x_all[0]
        mid_cols = hsh.shape[1] // 2

        def shared_part(k):
            cols = slice(k * mid_cols, (k + 1) * mid_cols)
            hsh[:, cols] = (jax.nn.silu(dot(xs, sg[:, cols])) * dot(xs, su[:, cols])).astype(BF16)

        scoped(relay, 0)
        scoped(relay, 1)
        shared_part(0)
        scoped(relay, 2)
        scoped(relay, 3)
        scoped(direct, n_blk - 1)
        shared_part(1)
        scoped(relay, 4)
        scoped(relay, 5)
        shared[...] = dot(hsh[...], sd[...]).astype(BF16)
    for k in range(2):
        scoped(finish, k)
    with jax.named_scope("drain"):
        await_all(x_all.at[0:3], ring_s)
        @pl.when(core == HUB)
        def _():
            await_all(x_all.at[0 : chips + 1], cross_s)

        @pl.when(core != HUB)
        def _():
            await_all(x_all.at[0 : chips - 1], cross_s)

        await_all(gt_send.at[0 : ep_size - 1], tile_s)
        await_all(d2d, d2d_s)
        await_all(tbuf.at[:, 0:3], ret_s)


def put_kernel(src, dst, o_sem):
    copy = pltpu.make_async_copy(src, dst, o_sem)
    copy.start()
    copy.wait()


def solution(mesh):
    ep_size = mesh.shape["ep"]

    def local_block(hidden_in, norm_gain, router_w, w_gate, w_up, w_down, ws_gate, ws_up, ws_down, expert_ids):
        tok, top_k = expert_ids.shape
        dim = hidden_in.shape[1]
        n_exp, _, inter = w_gate.shape
        s_inter = ws_gate.shape[1]
        cap = GROUPS * ((top_k + GROUP_LIMIT - 1) // GROUP_LIMIT) * tok // n_exp
        rows = ep_size * tok
        pairs = n_exp * cap
        n_blk = dim // COLS
        chips = ep_size // CORES
        vm, sem = pltpu.VMEM, pltpu.SemaphoreType.DMA
        scratch = [
            vm((tok, dim), BF16), vm((dim // 128, 128), F32), vm(router_w.shape, F32), vm((top_k, tok), jnp.int32),
            vm(w_gate.shape, BF16), vm(w_up.shape, BF16), vm(w_down.shape, BF16),
            vm(ws_gate.shape, BF16), vm(ws_up.shape, BF16), vm(ws_down.shape, BF16),
            vm((ep_size, tok, dim), BF16), vm((ep_size, n_exp, 128), F32), vm((ep_size, n_exp, 128), F32),
            vm((pairs, rows), BF16),
            vm((rows, 3 * pairs), BF16),
            vm((pairs, dim), BF16), vm((pairs, inter), BF16), vm((2, 3 * pairs, COLS), BF16),
            vm((8, CORES, chips * tok, COLS), F32), vm((n_blk, chips * tok, COLS), F32), vm((n_blk, chips, tok, COLS), F32),
            vm((n_blk, tok, COLS), F32), vm((n_blk, tok, COLS), F32), vm((n_blk, tok, COLS), F32), vm((n_blk, tok, COLS), F32),
            vm((tok, s_inter), BF16), vm((tok, dim), BF16),
            sem((4,)), sem((7,)), sem, sem, sem, sem, sem,
            sem((8,)), sem((5,)), sem, sem((n_blk,)), sem((n_blk,)), sem((2,)),
        ]
        result = pl.pallas_call(
            functools.partial(moe_kernel, ep_size, cap),
            out_shape=pltpu.VMEM((tok, dim), BF16),
            in_specs=[pl.BlockSpec(memory_space=pl.ANY)] * 10,
            out_specs=pl.BlockSpec(memory_space=pltpu.VMEM),
            scratch_shapes=scratch,
            compiler_params=pltpu.CompilerParams(collective_id=0, has_side_effects=True, vmem_limit_bytes=65_800_000),
            name="moe_block",
        )(hidden_in, norm_gain.reshape(dim // 128, 128), router_w, w_gate, w_up, w_down, ws_gate, ws_up, ws_down, expert_ids.T)
        return result

    row_spec = P(("dp", "ep"), None)
    in_specs = (row_spec, P(), P(), P("ep"), P("ep"), P("ep"), P(), P(), P(), row_spec)
    return jax.shard_map(local_block, mesh=mesh, in_specs=in_specs, out_specs=row_spec, check_vma=False)
```

```python
import functools

import jax
import jax.numpy as jnp
from jax import lax
from jax.experimental import pallas as pl
from jax.experimental.pallas import tpu as pltpu
from jax.sharding import PartitionSpec as P

NORM_EPS = 1e-6
ROUTE_SCALE = 2.5
GROUPS = 8
GROUP_LIMIT = 4
CORES = 2
HUB = 1
SPLIT = 4
S_ROW = (0, 1, 2, 4, 5, 6, 3, 7)
POS_OWN, POS_RIGHT, POS_LEFT, POS_FAR = range(4)
COLS = 256
CHUNK = 512
MESH = pl.DeviceIdType.MESH
F32 = jnp.float32
BF16 = jnp.bfloat16


def dot(a, b):
    return jnp.dot(a, b, preferred_element_type=F32)


def dot_t(a, b):
    return lax.dot_general(a, b, (((1,), (1,)), ((), ())), preferred_element_type=F32)


def split3(v):
    hi = v.astype(BF16)
    rest = v - hi.astype(F32)
    mid = rest.astype(BF16)
    low = (rest - mid.astype(F32)).astype(BF16)
    return hi, mid, low


def moe_kernel(ep_size, cap, hid_h, gain_h, rw_h, wg_h, wu_h, wd_h, sg_h, su_h, sd_h, ids_h, out_ref,
               hid, gain, rw, ids, wg, wu, wd, sg, su, sd, x_all, gt_send, gt_all, p_all, acat,
               xg, hbuf, ybuf, sbuf, d2d, tbuf, hop, rel, froml, fromr, hsh, shared,
               in_sem, w_sem,
               ring_s, cross_s, tile_s, d2d_s, ret_s, ag_r, cross_r, tile_r, d2d_r, hop_r, end_r):
    chips = ep_size // CORES
    tok, dim = hid.shape
    n_exp, _, inter = wg.shape
    top_k = ids.shape[0]
    half = dim // 2
    rows = ep_size * tok
    n_blk = dim // COLS
    hc = COLS // 2
    pairs = n_exp * cap

    me = lax.axis_index("ep")
    chip, core = me // CORES, me % CORES
    other = 1 - core
    right, left, opp = (chip + 1) % chips, (chip + chips - 1) % chips, (chip + 2) % chips

    def slot(a_chip, a_core, at_chip=chip, at_core=core):
        away = (a_chip - at_chip + chips) % chips
        pos = away + away // 2 - 2 * (away // 3)
        cross_core = (a_core + at_core) % CORES
        is_far = pos // POS_FAR
        return pos + (chips - 1) * cross_core + is_far * (chips - 1 - (chips - 2) * cross_core)

    def dev(a_chip, a_core):
        return {"ep": a_chip * CORES + a_core}

    def remote(src, dst, to, s_sem, r_sem):
        copy = pltpu.make_async_remote_copy(src, dst, s_sem, r_sem, device_id=to, device_id_type=MESH)
        copy.start()
        return copy

    def await_all(ref, sem):
        pltpu.make_async_copy(ref, ref, sem).wait()

    ins = [pltpu.make_async_copy(s, d, in_sem.at[i]) for i, (s, d) in enumerate(((hid_h, hid), (gain_h, gain), (rw_h, rw), (ids_h, ids)))]
    for copy in ins:
        copy.start()
    early, late = slice(0, COLS), slice(COLS, dim)
    chunk = (slice(0, CHUNK), slice(CHUNK, dim))
    fetches = [(h.at[:, rng, :], v.at[:, rng, :]) for rng in chunk for h, v in ((wg_h, wg), (wu_h, wu))]
    fetches += [(wd_h.at[:, :, early], wd.at[:, :, early]), (wd_h.at[:, :, late], wd.at[:, :, late]), (sg_h, sg), (su_h, su), (sd_h, sd)]
    weights = []
    for i, (s, d) in enumerate(fetches):
        weights.append(pltpu.make_async_copy(s, d, w_sem.at[min(i, 6)]))
        weights[-1].start(priority=1)

    barrier = pltpu.get_barrier_semaphore()
    for k in range(1, ep_size):
        pl.semaphore_signal(barrier, inc=1, device_id={"ep": (me + k) % ep_size}, device_id_type=MESH)

    with jax.named_scope("norm"):
        ins[0].wait()
        ins[1].wait()
        x_f32 = hid[...].astype(F32)
        inv_rms = lax.rsqrt(jnp.mean(x_f32 * x_f32, axis=-1, keepdims=True) + NORM_EPS)
        gain_row = jnp.concatenate([gain[i : i + 1, :] for i in range(dim // 128)], axis=1)
        x_norm = (x_f32 * inv_rms * gain_row).astype(BF16)
        x_all[0] = x_norm

    with jax.named_scope("barwait"):
        pl.semaphore_wait(barrier, ep_size - 1)

    side_a = [slice(0, CHUNK // 2), slice(CHUNK, (CHUNK + dim) // 2)]
    side_b = [slice(CHUNK // 2, CHUNK), slice((CHUNK + dim) // 2, dim)]

    def spread(a_chip, cols, to, r_sem, to_core=core):
        src, dst = x_all.at[slot(a_chip, core), :, cols], x_all.at[slot(a_chip, core, to, to_core), :, cols]
        return remote(src, dst, dev(to, to_core), ring_s, r_sem)

    def cross(a_chip, cols, r_sem):
        src, dst = x_all.at[slot(a_chip, core), :, cols], x_all.at[slot(a_chip, core, chip, other), :, cols]
        remote(src, dst, dev(chip, other), cross_s, r_sem)

    ra, lb = [], []

    def own_rows(k):
        ra.append(spread(chip, side_a[k], right, ag_r.at[k]))
        lb.append(spread(chip, side_b[k], left, ag_r.at[2 + k]))
        spread(chip, side_b[k], right, ag_r.at[4 + k])
        spread(chip, side_a[k], left, ag_r.at[4 + k])

    own_rows(0)
    cross(chip, slice(0, dim), cross_r.at[0])

    with jax.named_scope("router"):
        ins[2].wait()
        ins[3].wait()
        n_all = rw.shape[0]
        terms = dot_t(jnp.concatenate(split3(rw[...]), axis=0), x_norm)
        logits = (terms[2 * n_all :, :] + terms[n_all : 2 * n_all, :]) + terms[:n_all, :]
        scores = 1.0 / (1.0 + jnp.exp(-logits))
        exp_no = lax.broadcasted_iota(jnp.int32, logits.shape, 0)
        chosen = exp_no == ids[0:1, :]
        for k in range(1, top_k):
            chosen = jnp.logical_or(chosen, exp_no == ids[k : k + 1, :])
        total = jnp.sum(jnp.where(chosen, scores, 0.0), axis=0, keepdims=True)
        gates = jnp.where(chosen, ROUTE_SCALE * scores / total, -1.0)
        gt_send[...] = jnp.full(gt_send.shape, -1.0, F32)
        for d in range(ep_size):
            gt_send[d, :, 0:tok] = gates[d * n_exp : (d + 1) * n_exp, :]
        gt_all[0] = gt_send[me]
        for k in range(1, ep_size):
            to = (me + k) % ep_size
            remote(gt_send.at[to], gt_all.at[slot(chip, core, to // CORES, to % CORES)], {"ep": to}, tile_s, tile_r)

    own_rows(1)

    def pass_on(k):
        with jax.named_scope(f"relays{k}"):
            ra[k].wait_recv()
            spread(left, side_a[k], right, ag_r.at[6 + k], HUB)
            cross(left, side_a[k], cross_r.at[1 + k])
            lb[k].wait_recv()
            spread(right, side_b[k], left, ag_r.at[6 + k], HUB)
            cross(right, side_b[k], cross_r.at[1 + k])

    pass_on(0)

    def near_rest(k):
        with jax.named_scope(f"rest{k}"):
            await_all(x_all.at[0, :, chunk[k]], ag_r.at[4 + k])
            cross(left, side_b[k], cross_r.at[1 + k])
            cross(right, side_a[k], cross_r.at[1 + k])

    with jax.named_scope("tilewait"):
        await_all(gt_all.at[0 : ep_size - 1], tile_r)

    with jax.named_scope("onehot"):
        lane_src = lax.broadcasted_iota(jnp.int32, (n_exp, rows), 1) // tok
        gmat = jnp.full((n_exp, rows), -1.0, F32)
        for s in range(ep_size):
            wide = jnp.concatenate([gt_all[s], jnp.full((n_exp, rows - gt_all.shape[2]), -1.0, F32)], axis=1)
            if s:
                wide = pltpu.roll(wide, s * tok, 1)
            gmat = jnp.where(lane_src == s, wide, gmat)
        picked = jnp.logical_not(gmat < 0.0)
        upper = lax.broadcasted_iota(jnp.int32, (rows, rows), 0) < lax.broadcasted_iota(jnp.int32, (rows, rows), 1)
        rank = dot(jnp.where(picked, 1.0, 0.0).astype(BF16), jnp.where(upper, 1.0, 0.0).astype(BF16))
        place = jnp.where(picked, rank, -1.0)
        for i in range(pairs // 128):
            e_one, e_two = i * 128 // cap, (i * 128 + 127) // cap
            row_no = lax.broadcasted_iota(jnp.int32, (128, rows), 0) + i * 128
            first = row_no < e_two * cap
            pos = (row_no - jnp.where(first, e_one * cap, e_two * cap)).astype(F32)
            hit = pos == jnp.where(first, place[e_one : e_one + 1, :], place[e_two : e_two + 1, :])
            gated = jnp.where(hit, jnp.where(first, gmat[e_one : e_one + 1, :], gmat[e_two : e_two + 1, :]), 0.0)
            p_all[i * 128 : (i + 1) * 128, :] = jnp.where(hit, 1.0, 0.0).astype(BF16)
            for k, term in enumerate(reversed(split3(gated.T))):
                for b in range(ep_size):
                    to_row = S_ROW[b] * tok
                    acat[to_row : to_row + tok, k * pairs + i * 128 : k * pairs + (i + 1) * 128] = term[b * tok : (b + 1) * tok, :]

    n_near = rows // 2
    with jax.named_scope("nearwait"):
        await_all(x_all.at[0], cross_r.at[0])
    x_near = x_all.at[0 : ep_size // 2]
    x_rest = x_all.at[ep_size // 2 : ep_size]

    far_slots = slice(ep_size - CORES, ep_size)

    def far_wait(k):
        @pl.when(core != HUB)
        def _():
            await_all(x_all.at[far_slots, :, chunk[k]], cross_r.at[3 + k])

    def gather_near(k):
        with jax.named_scope(f"near{k}"):
            xg[:, chunk[k]] = dot(p_all[:, 0:n_near], x_near[:, :, chunk[k]].reshape(n_near, -1)).astype(BF16)

    def pass_far(k):
        with jax.named_scope(f"far{k}"):
            @pl.when(core == HUB)
            def _():
                await_all(x_all.at[far_slots, :, chunk[k]], ag_r.at[6 + k])
                for i in range(CORES):
                    src, dst = x_all.at[ep_size - 1 - i, :, chunk[k]], x_all.at[ep_size - CORES + i, :, chunk[k]]
                    remote(src, dst, dev(chip, other), cross_s, cross_r.at[3 + k])

    def gate_up(k, first, end):
        def gather_far(p):
            two = slice(2 * p * cap, 2 * (p + 1) * cap)
            xg[two, chunk[k]] = xg[two, chunk[k]] + dot(p_all[two, n_near:], x_rest[:, :, chunk[k]].reshape(rows - n_near, -1)).astype(BF16)

        gather_far(first // 2)
        for e in range(first, end):
            if e % 2 == 0 and e + 2 < end:
                gather_far(e // 2 + 1)
            own = slice(e * cap, (e + 1) * cap)
            row = e % 4 * cap
            xe = xg[own, chunk[k]]
            h = []
            for m, w in enumerate((wg, wu)):
                total_h = dot(xe, w[e, chunk[k], :])
                for c in range(2):
                    spot = sbuf.at[4 * m + 2 * c + e // 4, row // (chips * tok), row % (chips * tok) : row % (chips * tok) + cap, :]
                    piece = total_h[:, c * COLS : (c + 1) * COLS]
                    if k == 0:
                        spot[...] = piece
                    else:
                        h.append(spot[...] + piece)
            if k:
                for c in range(2):
                    hbuf[own, c * COLS : (c + 1) * COLS] = (jax.nn.silu(h[c]) * h[2 + c]).astype(BF16)

    pass_on(1)
    near_rest(0)
    gather_near(0)
    near_rest(1)
    pass_far(0)
    gather_near(1)
    with jax.named_scope("farwait0"):
        await_all(x_all.at[0 : chips - 2, :, chunk[0]], cross_r.at[1])
        far_wait(0)
        weights[0].wait()
        weights[1].wait()
    with jax.named_scope("gateup0"):
        gate_up(0, 0, SPLIT)
    pass_far(1)
    with jax.named_scope("gateup0b"):
        gate_up(0, SPLIT, n_exp)
    with jax.named_scope("farwait1"):
        await_all(x_all.at[0 : chips - 2, :, chunk[1]], cross_r.at[2])
        far_wait(1)
        for copy in weights[2:5]:
            copy.wait()

    part = []

    def last(j):
        cols = slice(j * COLS, (j + 1) * COLS)
        for e in range(n_exp):
            y = dot(hbuf[e * cap : (e + 1) * cap, :], wd[e, :, cols]).astype(BF16)
            for k in range(3):
                ybuf[j % 2, k * pairs + e * cap : k * pairs + (e + 1) * cap, :] = y

    def compute(j):
        if j == 1:
            last(1)
        if j and j + 1 < n_blk:
            last(j + 1)
        for k in range(CORES):
            sbuf[j, k] = dot(acat[k * chips * tok : (k + 1) * chips * tok, :], ybuf[j % 2])
        part.append(remote(sbuf.at[j, 1], d2d.at[j], dev(chip, other), d2d_s, d2d_r.at[j]))

    lo, up = slice(0, hc), slice(hc, COLS)
    late_blk = n_blk - 1

    def send(j):
        part[j].wait_recv()
        tbuf[j] = (sbuf[j, 0] + d2d[j]).reshape(chips, tok, COLS)
        remote(tbuf.at[j, POS_FAR, :, lo], hop.at[j, :, lo], dev(right, core), ret_s, hop_r.at[j])
        remote(tbuf.at[j, POS_FAR, :, up], hop.at[j, :, up], dev(left, core), ret_s, hop_r.at[j])

    def direct(j):
        remote(tbuf.at[j, POS_RIGHT, :, up], froml.at[j, :, up], dev(right, core), ret_s, end_r.at[j // late_blk])
        remote(tbuf.at[j, POS_LEFT, :, lo], fromr.at[j, :, lo], dev(left, core), ret_s, end_r.at[j // late_blk])

    def relay(j):
        await_all(hop.at[j], hop_r.at[j])
        rel[j, :, lo] = hop[j, :, lo] + tbuf[j, POS_RIGHT, :, lo]
        rel[j, :, up] = hop[j, :, up] + tbuf[j, POS_LEFT, :, up]
        remote(rel.at[j, :, lo], froml.at[j, :, lo], dev(right, core), ret_s, end_r.at[j // late_blk])
        remote(rel.at[j, :, up], fromr.at[j, :, up], dev(left, core), ret_s, end_r.at[j // late_blk])

    def finish(k):
        blks = range(late_blk) if k == 0 else range(late_blk, n_blk)
        await_all(tbuf.at[blks[0] : blks[-1] + 1, 0:2], end_r.at[k])
        for j in blks:
            cols = slice(j * COLS, (j + 1) * COLS)
            routed = (tbuf[j, POS_OWN] + froml[j]) + fromr[j]
            out_ref[:, cols] = ((hid[:, cols].astype(F32) + shared[:, cols].astype(F32)) + routed).astype(BF16)

    def scoped(f, j):
        with jax.named_scope(f"{f.__name__}{j}"):
            f(j)

    with jax.named_scope("gateup1"):
        gate_up(1, 0, n_exp)
        last(0)
        compute(0)
    weights[5].wait()
    for j in range(n_blk):
        if j:
            scoped(compute, j)
        if j >= 1:
            scoped(send, j - 1)
            scoped(direct, j - 1)
    scoped(send, n_blk - 1)

    with jax.named_scope("shared"):
        await_all(wg.at[0 : 3 * sd.shape[0] // inter], w_sem.at[6])
        xs = x_all[0]
        mid_cols = hsh.shape[1] // 2

        def shared_part(k):
            cols = slice(k * mid_cols, (k + 1) * mid_cols)
            hsh[:, cols] = (jax.nn.silu(dot(xs, sg[:, cols])) * dot(xs, su[:, cols])).astype(BF16)

        scoped(relay, 0)
        scoped(relay, 1)
        shared_part(0)
        scoped(relay, 2)
        scoped(relay, 3)
        scoped(direct, n_blk - 1)
        shared_part(1)
        scoped(relay, 4)
        scoped(relay, 5)
        shared[...] = dot(hsh[...], sd[...]).astype(BF16)
    for k in range(2):
        scoped(finish, k)
    with jax.named_scope("drain"):
        await_all(x_all.at[0:3], ring_s)
        @pl.when(core == HUB)
        def _():
            await_all(x_all.at[0 : chips + 1], cross_s)

        @pl.when(core != HUB)
        def _():
            await_all(x_all.at[0 : chips - 1], cross_s)

        await_all(gt_send.at[0 : ep_size - 1], tile_s)
        await_all(d2d, d2d_s)
        await_all(tbuf.at[:, 0:3], ret_s)


def put_kernel(src, dst, o_sem):
    copy = pltpu.make_async_copy(src, dst, o_sem)
    copy.start()
    copy.wait()


def solution(mesh):
    ep_size = mesh.shape["ep"]

    def local_block(hidden_in, norm_gain, router_w, w_gate, w_up, w_down, ws_gate, ws_up, ws_down, expert_ids):
        tok, top_k = expert_ids.shape
        dim = hidden_in.shape[1]
        n_exp, _, inter = w_gate.shape
        s_inter = ws_gate.shape[1]
        cap = GROUPS * ((top_k + GROUP_LIMIT - 1) // GROUP_LIMIT) * tok // n_exp
        rows = ep_size * tok
        pairs = n_exp * cap
        n_blk = dim // COLS
        chips = ep_size // CORES
        vm, sem = pltpu.VMEM, pltpu.SemaphoreType.DMA
        scratch = [
            vm((tok, dim), BF16), vm((dim // 128, 128), F32), vm(router_w.shape, F32), vm((top_k, tok), jnp.int32),
            vm(w_gate.shape, BF16), vm(w_up.shape, BF16), vm(w_down.shape, BF16),
            vm(ws_gate.shape, BF16), vm(ws_up.shape, BF16), vm(ws_down.shape, BF16),
            vm((ep_size, tok, dim), BF16), vm((ep_size, n_exp, 128), F32), vm((ep_size, n_exp, 128), F32),
            vm((pairs, rows), BF16),
            vm((rows, 3 * pairs), BF16),
            vm((pairs, dim), BF16), vm((pairs, inter), BF16), vm((2, 3 * pairs, COLS), BF16),
            vm((8, CORES, chips * tok, COLS), F32), vm((n_blk, chips * tok, COLS), F32), vm((n_blk, chips, tok, COLS), F32),
            vm((n_blk, tok, COLS), F32), vm((n_blk, tok, COLS), F32), vm((n_blk, tok, COLS), F32), vm((n_blk, tok, COLS), F32),
            vm((tok, s_inter), BF16), vm((tok, dim), BF16),
            sem((4,)), sem((7,)), sem, sem, sem, sem, sem,
            sem((8,)), sem((5,)), sem, sem((n_blk,)), sem((n_blk,)), sem((2,)),
        ]
        result = pl.pallas_call(
            functools.partial(moe_kernel, ep_size, cap),
            out_shape=pltpu.VMEM((tok, dim), BF16),
            in_specs=[pl.BlockSpec(memory_space=pl.ANY)] * 10,
            out_specs=pl.BlockSpec(memory_space=pltpu.VMEM),
            scratch_shapes=scratch,
            compiler_params=pltpu.CompilerParams(collective_id=0, has_side_effects=True, vmem_limit_bytes=65_800_000),
            name="moe_block",
        )(hidden_in, norm_gain.reshape(dim // 128, 128), router_w, w_gate, w_up, w_down, ws_gate, ws_up, ws_down, expert_ids.T)
        return result

    row_spec = P(("dp", "ep"), None)
    in_specs = (row_spec, P(), P(), P("ep"), P("ep"), P("ep"), P(), P(), P(), row_spec)
    return jax.shard_map(local_block, mesh=mesh, in_specs=in_specs, out_specs=row_spec, check_vma=False)
```
